32 devices in a mesh: gx: 4 (over z), gy: 8 (over y, x, core).
Axes of the slice: x: 2, y: 2, z: 4, core: 2. Of those that a mesh axis runs over, the one named last changes fastest.
Arguments:
- gradient: float32 [32, 2048], P('gx', 'gy'), may hold values from -6 to 6
- warm_start: float32 [32, 2048], P('gx', 'gy'), may hold values from -3 to 3
- viscosity: float32 [32, 32, 2048], P(None, 'gx', 'gy'), may hold values from 1 to 10
- friction_coef: float32 [32, 2048], P('gx', 'gy'), may hold values from 0.5 to 5
- slide_dir: float32 [2, 32, 2048], P(None, 'gx', 'gy'), may hold values from -4 to 4
- obs_weight: float32 [32, 2048], P('gx', 'gy'), may hold values from 0.5 to 2
- ice_mask: int32 [32, 2048], P('gx', 'gy'), may hold values 0 or 1
- grounded: int32 [32, 2048], P('gx', 'gy'), may hold values 0 or 1
Outputs:
- solution: float32 [32, 2048], P('gx', 'gy')
- residual: float32 [32, 2048], P('gx', 'gy')
The draws below stay inside these ranges and needn't reach their ends.
All inputs are finite; a program needn't handle non-finite values. No bound on the sum of `ice_mask` or of `grounded` on one device may be relied on, other than what follows from the above.
Results may differ from the reference program's by a relative error of at most 0.00075.
Values sent between devices are 32-bit elements; how exact they have to be, the bound alone decides.
A program may use at most 128 MiB of HBM per device.

```python
import math
import jax
import jax.numpy as jnp

NZ = 32
ITERS = 2
NX = 32
NY = 2048


def plant(entries, rng, smallest, high):
    spot = [jax.random.randint(jax.random.fold_in(rng, axis), (), 0, length) for axis, length in enumerate(entries.shape)]
    longest = entries.shape.index(max(entries.shape))
    neighbour = spot[:longest] + [(spot[longest] + 1) % entries.shape[longest]] + spot[longest + 1:]
    return entries.at[tuple(spot)].set(smallest).at[tuple(neighbour)].set(high)


def block_levels(own_key, dims, shards, smallest, high):
    def one(dim, parts):
        steps = jax.random.uniform(jax.random.fold_in(jax.random.fold_in(own_key, 6), dim), (parts,), jnp.float32, smallest / len(shards), high / len(shards))
        return jnp.repeat(jnp.exp(steps), dims[dim] // parts).reshape((-1,) + (1,) * (len(dims) - dim - 1))

    gain = one(*shards[0])
    for cut in shards[1:]:
        gain = gain * one(*cut)
    return gain


def normal_values(key, dims, scale, limit, pieces=(), kind=jnp.bfloat16):
    values = jax.random.normal(key, dims, jnp.float32) * scale
    if len(pieces) > 0:
        values = block_levels(key, dims, pieces, -0.22, 0.18) * values
    return jnp.clip(values, min=-limit, max=limit).astype(kind)


def setup_inputs(seed: int = 0) -> dict:
    keys = jax.random.split(jax.random.key(seed), 9)
    gradient = normal_values(keys[0], (NX, NY), 1.0, 6.0, ((0, 4), (1, 8)), jnp.float32)
    warm_start = normal_values(keys[1], (NX, NY), 0.5, 3.0, ((0, 4), (1, 8)), jnp.float32)
    viscosity = jnp.clip(jnp.exp(math.log(10.0) - 2.3025851 * jax.random.uniform(keys[2], (NZ, NX, NY), jnp.float32) ** block_levels(keys[2], (NZ, NX, NY), ((1, 4), (2, 8)), -0.2, 0.2)), 1.0, 10.0)
    friction_coef = jnp.clip(jnp.exp(math.log(5.0) - 2.3025851 * jax.random.uniform(keys[3], (NX, NY), jnp.float32) ** block_levels(keys[3], (NX, NY), ((0, 4), (1, 8)), -0.2, 0.2)), 0.5, 5.0)
    slide_dir = normal_values(keys[4], (2, NX, NY), 1.0, 4.0, ((1, 4), (2, 8)), jnp.float32)
    obs_weight = jnp.clip(jnp.exp(math.log(2.0) - 1.3862944 * jax.random.uniform(keys[5], (NX, NY), jnp.float32) ** block_levels(keys[5], (NX, NY), ((0, 4), (1, 8)), -0.2, 0.2)), 0.5, 2.0)
    ice_mask = plant((jax.random.randint(keys[6], (NX, NY), 0, 8) < 7).astype(jnp.int32), jax.random.fold_in(keys[6], 1), 0, 1)
    grounded = plant((jax.random.randint(keys[7], (NX, NY), 0, 4) < 3).astype(jnp.int32), jax.random.fold_in(keys[7], 1), 0, 1)
    return {"gradient": gradient, "warm_start": warm_start, "viscosity": viscosity, "friction_coef": friction_coef, "slide_dir": slide_dir, "obs_weight": obs_weight, "ice_mask": ice_mask, "grounded": grounded}


vert_coupling = 128.0
sink_rate = 0.0625
bed_drag = 0.5
offset_weight = 0.0019
cross_share = 0.5
reg_gamma = 0.02
reg_smooth = 1.0
diag_scale = 0.003

neighbour_offsets = [(step_z, step_x, step_y) for step_z in (-1, 0, 1) for step_x in (-1, 0, 1) for step_y in (-1, 0, 1) if step_x != 0 or step_y != 0]


def couple(field_ext, eta_ext):
    levels = eta_ext.shape[0]
    span_x = eta_ext.shape[1] - 2
    span_y = eta_ext.shape[2] - 2
    padded_field = jnp.pad(field_ext, ((0, 0), (1, 1), (0, 0), (0, 0)))
    padded_eta = jnp.pad(eta_ext, ((1, 1), (0, 0), (0, 0)))
    center = eta_ext[:, 1:1 + span_x, 1:1 + span_y]
    along_one = jnp.zeros((levels, span_x, span_y), jnp.float32)
    along_two = jnp.zeros((levels, span_x, span_y), jnp.float32)
    for step_z, step_x, step_y in neighbour_offsets:
        near_eta = padded_eta[1 + step_z:1 + step_z + levels, 1 + step_x:1 + step_x + span_x, 1 + step_y:1 + step_y + span_y]
        weight = (offset_weight / (abs(step_x) + abs(step_y) + abs(step_z))) * 0.5 * (center + near_eta)
        near_field = padded_field[:, 1 + step_z:1 + step_z + levels, 1 + step_x:1 + step_x + span_x, 1 + step_y:1 + step_y + span_y]
        along_one = along_one + weight * near_field[0]
        along_two = along_two + weight * near_field[1]
        if step_x != 0 and step_y != 0:
            twist_weight = (cross_share * step_x * step_y) * weight
            along_one = along_one + twist_weight * near_field[1]
            along_two = along_two + twist_weight * near_field[0]
    return jnp.stack([along_one, along_two])


def tridiagonal(link_weights, diagonal, rhs_cols):
    levels = diagonal.shape[0]
    pivot_value = diagonal[0]
    ratios = [-link_weights[0] / pivot_value]
    partial_value = [rhs_cols[:, 0] / pivot_value]
    for layer_index in range(1, levels):
        pivot_value = diagonal[layer_index] + link_weights[layer_index - 1] * ratios[-1]
        partial_value.append((rhs_cols[:, layer_index] + link_weights[layer_index - 1] * partial_value[-1]) / pivot_value)
        if layer_index < levels - 1:
            ratios.append(-link_weights[layer_index] / pivot_value)
    result = [partial_value[-1]]
    for layer_index in range(levels - 2, -1, -1):
        result.insert(0, partial_value[layer_index] - ratios[layer_index] * result[0])
    return jnp.stack(result, axis=1)


def responses(viscosity, friction):
    levels = viscosity.shape[0]
    link_weights = vert_coupling * 0.5 * (viscosity[:-1] + viscosity[1:])
    zero_layer = jnp.zeros_like(viscosity[:1])
    diagonal = jnp.concatenate([zero_layer, link_weights]) + jnp.concatenate([link_weights, zero_layer]) + sink_rate * viscosity
    diagonal = diagonal.at[0].add(bed_drag * friction)
    unit_rhs = jnp.zeros((2,) + viscosity.shape, jnp.float32)
    unit_rhs = unit_rhs.at[0, 0].set(1.0).at[1, levels - 1].set(1.0)
    solved = tridiagonal(link_weights, diagonal, unit_rhs)
    return solved[0], solved[1]


def regularize(centre_ext):
    middle = centre_ext[1:-1, 1:-1]
    beside_all = centre_ext[2:, 1:-1] + centre_ext[:-2, 1:-1] + centre_ext[1:-1, 2:] + centre_ext[1:-1, :-2]
    return reg_gamma * (middle + reg_smooth * (4.0 * middle - beside_all))


def reference(gradient, warm_start, viscosity, friction_coef, slide_dir, obs_weight, ice_mask, grounded):
    ice_float = ice_mask.astype(jnp.float32)
    ground_float = grounded.astype(jnp.float32)
    friction = ground_float * friction_coef
    source = (ice_float * ground_float * friction_coef)[None] * slide_dir
    obs = ice_float * obs_weight
    inverse_diag = 1.0 / (reg_gamma * (1.0 + 4.0 * reg_smooth) + diag_scale * ice_float * ground_float * friction_coef * friction_coef)
    bottom_resp, top_resp = responses(viscosity, friction)
    eta_ext = jnp.pad(viscosity, ((0, 0), (1, 1), (1, 1)))

    def hessian(direction):
        spread = source * direction[None]
        first_state = bottom_resp[None] * spread[:, None]
        coupled = couple(jnp.pad(first_state, ((0, 0), (0, 0), (1, 1), (1, 1))), eta_ext)
        surface = spread * bottom_resp[-1][None] + jnp.sum(top_resp[None] * coupled, axis=1)
        traction = obs[None] * surface
        second_state = top_resp[None] * traction[:, None]
        coupled_back = couple(jnp.pad(second_state, ((0, 0), (0, 0), (1, 1), (1, 1))), eta_ext)
        basal_part = traction * top_resp[0][None] + jnp.sum(bottom_resp[None] * coupled_back, axis=1)
        return jnp.sum(source * basal_part, axis=0) + regularize(jnp.pad(direction, 1))

    solution = warm_start
    residual = gradient - hessian(warm_start)
    precond = inverse_diag * residual
    direction = precond
    norm_now = jnp.sum(residual * precond)
    for iteration in range(ITERS):
        image_vec = hessian(direction)
        step_size = norm_now / jnp.sum(direction * image_vec)
        solution = solution + step_size * direction
        residual = residual - step_size * image_vec
        precond = inverse_diag * residual
        norm_next = jnp.sum(residual * precond)
        direction = precond + (norm_next / norm_now) * direction
        norm_now = norm_next
    return solution, residual
```

```python
import functools

import jax
import jax.numpy as jnp
from jax import lax
from jax.experimental import pallas as pl
from jax.experimental.pallas import tpu as pltpu
from jax.sharding import PartitionSpec as P

vert_coupling = 128.0
sink_rate = 0.0625
bed_drag = 0.5
offset_weight = 0.0019
cross_share = 0.5
reg_gamma = 0.02
reg_smooth = 1.0
diag_scale = 0.003

MESH = pl.DeviceIdType.MESH
LOGICAL = pl.DeviceIdType.LOGICAL
REACH = 6
DIRS = [(-1, 0), (1, 0), (0, -1), (0, 1), (-1, -1), (-1, 1), (1, -1), (1, 1)]
OPPOSITE = [1, 0, 3, 2, 7, 6, 5, 4]
FIELDS = 7


def roll(x, shift, axis):
    size = x.shape[axis]
    if isinstance(shift, int):
        shift = shift % size
        if shift == 0:
            return x
    return pltpu.roll(x, shift, axis)


def near(x, step, axis):
    return roll(x, -step, axis)


def kernel(
    nx, ny,
    grad_in, warm_in, visc_in, fric_in, slide_in, obs_in, ice_in, ground_in,
    out_ref,
    grad_ref, warm_ref, visc_ref, fric_ref, slide_ref, obs_ref, ice_ref, ground_ref,
    up, down, bot, gbot, top, gtop,
    t_row, row_send, row_recv, f_send, f_recv, p_send, p_recv, k_send, k_recv, kp_send, kp_recv,
    ext, red, slots,
    load_sem, s_send, s_recv, r_send, r_recv, all_in,
):
    levels, rows, cols = visc_ref.shape
    n = nx * ny
    ix, iy = lax.axis_index("gx"), lax.axis_index("gy")
    me = ix * ny + iy

    loads = [
        pltpu.make_async_copy(src, dst, load_sem.at[j])
        for j, (src, dst) in enumerate((
            (visc_in, visc_ref), (fric_in, fric_ref), (ground_in, ground_ref), (ice_in, ice_ref),
            (slide_in, slide_ref), (obs_in, obs_ref), (warm_in, warm_ref), (grad_in, grad_ref),
        ))
    ]

    def exists(d):
        dx, dy = DIRS[d]
        x, y = ix + dx, iy + dy
        return (x >= 0) & (x < nx) & (y >= 0) & (y < ny)

    barrier = pltpu.get_barrier_semaphore()

    def greet(x, y):
        pl.semaphore_signal(barrier, inc=1, device_id=(x, y), device_id_type=MESH)

    for load in loads:
        load.start()
    expected = nx - 1 + ny - 1
    for d in range(4, 8):
        expected = expected + exists(d).astype(jnp.int32)

        @pl.when(exists(d))
        def _():
            greet(ix + DIRS[d][0], iy + DIRS[d][1])
    for k in range(1, nx):
        greet(lax.rem(ix + k, nx), iy)
    for k in range(1, ny):
        greet(ix, lax.rem(iy + k, ny))

    def copy(src, dst, d, sem):
        dx, dy = DIRS[d]
        return pltpu.make_async_remote_copy(
            src_ref=src, dst_ref=dst,
            send_sem=s_send.at[sem + d], recv_sem=s_recv.at[sem + OPPOSITE[d]],
            device_id=(jnp.clip(ix + dx, 0, nx - 1), jnp.clip(iy + dy, 0, ny - 1)),
            device_id_type=MESH,
        )

    def message(d, what):
        o = OPPOSITE[d]
        side = 0 if DIRS[d][1] < 0 else 1
        return {
            "row": lambda: copy(row_send.at[d], row_recv.at[o], d, 0),
            "field": lambda: copy(f_send, f_recv.at[o], d, 8),
            "coef": lambda: copy(k_send, k_recv.at[o], d, 16),
            "pack": lambda: copy(p_send.at[side], p_recv.at[o - 2], d, 0),
            "coefpack": lambda: copy(kp_send.at[side], kp_recv.at[o - 2], d, 16),
        }[what]()

    beside_x, others = (0, 1), range(2, 8)
    kinds = (("row", beside_x), ("pack", others), ("field", beside_x), ("coefpack", others), ("coef", beside_x))

    def each(action, names):
        for name, towards in kinds:
            if name not in names:
                continue
            for d in towards:
                @pl.when(exists(d))
                def _():
                    if action == "wait_recv":
                        message(OPPOSITE[d], name).wait_recv()
                    elif action == "wait_send":
                        message(d, name).wait_send()
                    else:
                        message(d, name).start()

    def clear(ref):
        ref[...] = jnp.zeros(ref.shape, jnp.float32)

    for d in range(8):
        @pl.when(jnp.logical_not(exists(d)))
        def _():
            for ref in (row_recv, f_recv, k_recv) if d < 2 else (p_recv, kp_recv):
                clear(ref.at[d if d < 2 else d - 2])

    for load in loads:
        load.wait()

    ice = ice_ref[...].astype(jnp.float32)
    ground = ground_ref[...].astype(jnp.float32)
    fric = fric_ref[...]
    friction = ground * fric
    base = ice * ground * fric
    inverse = 1.0 / (reg_gamma * (1.0 + 4.0 * reg_smooth) + diag_scale * base * fric)
    lane = lax.broadcasted_iota(jnp.int32, (rows, 128), 1)

    def eliminate(i, carry):
        e, f = carry
        k = levels - 2 - i
        v_low, v_up = visc_ref[i], visc_ref[i + 1]
        link = (vert_coupling * 0.5) * (v_low + v_up)
        ratio = link / (link + e)
        up[i] = ratio
        e = sink_rate * v_up + e * ratio
        w_low, w_up = visc_ref[k], visc_ref[k + 1]
        link = (vert_coupling * 0.5) * (w_low + w_up)
        ratio = link / (link + f)
        down[k] = ratio
        f = sink_rate * w_low + f * ratio
        return e, f

    e = sink_rate * visc_ref[0] + bed_drag * friction
    f = sink_rate * visc_ref[levels - 1]
    e, f = lax.fori_loop(0, levels - 1, eliminate, (e, f), unroll=True)

    zero = jnp.zeros((rows, cols), jnp.float32)
    for ref in (top, gtop):
        ref[0] = zero
        ref[levels + 1] = zero

    def respond(z, carry):
        b, t, left, right, tleft, tright = carry
        g = visc_ref[z] * b
        bot[z] = b
        gbot[z] = g
        for j, val in ((0, b), (levels, g)):
            row_send[0, pl.ds(z + j, 1), :] = val[:1]
            row_send[1, pl.ds(z + j, 1), :] = val[rows - 1:]
            left = jnp.where(lane == z + j, roll(val[:, :128], z + j, 1), left)
            right = jnp.where(lane == z + j, roll(val[:, cols - 128:], z + j + 1, 1), right)
        k = levels - 1 - z
        top[k + 1] = t
        h = visc_ref[k] * t
        gtop[k + 1] = h
        for j, val in ((0, h), (levels, t)):
            t_row[0, pl.ds(k + j, 1), :] = val[:1]
            t_row[1, pl.ds(k + j, 1), :] = val[rows - 1:]
            tleft = jnp.where(lane == k + j, roll(val[:, :128], k + j, 1), tleft)
            tright = jnp.where(lane == k + j, roll(val[:, cols - 128:], k + j + 1, 1), tright)
        t = t * up[jnp.maximum(k - 1, 0)]
        b = b * down[jnp.minimum(z, levels - 2)]
        return b, t, left, right, tleft, tright

    blank = jnp.zeros((rows, 128), jnp.float32)
    _, _, left, right, tleft, tright = lax.fori_loop(
        0, levels, respond, (1.0 / (f + bed_drag * friction), 1.0 / e, blank, blank, blank, blank), unroll=4
    )

    own = [base * slide_ref[0], base * slide_ref[1], ice * obs_ref[...], inverse, bot[levels - 1], warm_ref[...], grad_ref[...]]

    def pack(fields, place, left, right):
        for val in fields:
            here = (lane >= place) & (lane < place + REACH)
            left = jnp.where(here, roll(val[:, :128], place, 1), left)
            right = jnp.where(here, roll(val[:, cols - 128:], place - (128 - REACH), 1), right)
            place += REACH
        return left, right

    left, right = pack(own, 2 * levels, left, right)
    for j, val in enumerate(own):
        f_send[j] = val
    p_send[0] = left
    p_send[1] = right

    pl.semaphore_wait(barrier, expected)
    each("start", ("row", "pack", "field"))
    for k in range(1, ny):
        pl.semaphore_signal(all_in, inc=1, device_id=(ix, lax.rem(iy + k, ny)), device_id_type=MESH)

    row_id = lax.broadcasted_iota(jnp.int32, (rows, cols), 0)
    col_id = lax.broadcasted_iota(jnp.int32, (rows, cols), 1)
    prow = lax.broadcasted_iota(jnp.int32, (rows, 128), 0)

    def beside(side):
        at = {dx: p_recv[DIRS.index((dx, side)) - 2] for dx in (-1, 0, 1)}
        return {
            -1: jnp.where(prow == 0, near(at[-1], -1, 0), near(at[0], -1, 0)),
            0: at[0],
            1: jnp.where(prow == rows - 1, near(at[1], 1, 0), near(at[0], 1, 0)),
        }

    def weigh(mid, out):
        return (
            (0.5 * offset_weight) * mid + (0.25 * offset_weight) * out,
            (0.25 * offset_weight) * mid + (0.5 * offset_weight / 3.0) * out,
        )

    def gather(z, acc):
        acc = list(acc)
        weights = [weigh(ref[z + 1], ref[z] + ref[z + 2]) for ref in (gtop, top)]
        for ref, weight in ((bot, weights[0]), (gbot, weights[1])):
            mid = ref[z]
            low = jnp.where(row_id == 0, 0.0, near(mid, -1, 0))
            high = jnp.where(row_id == rows - 1, 0.0, near(mid, 1, 0))
            for dx, val in ((-1, low), (0, mid), (1, high)):
                for dy in (-1, 0, 1):
                    if (dx, dy) != (0, 0):
                        d = DIRS.index((dx, dy))
                        moved = val if dy == 0 else near(val, dy, 1)
                        acc[d] = acc[d] + weight[1 if dx * dy != 0 else 0] * moved
        return tuple(acc)

    coefs = list(lax.fori_loop(0, levels, gather, (zero,) * 8, unroll=4))
    for d, (dx, dy) in enumerate(DIRS):
        if dy != 0:
            coefs[d] = jnp.where(col_id == (0 if dy < 0 else cols - 1), 0.0, coefs[d])

    layer = lax.broadcasted_iota(jnp.int32, (2 * levels, cols), 0)
    edge_col = lax.broadcasted_iota(jnp.int32, (2 * levels, cols), 1)

    def above_below(mid, index, axis):
        low = (index == 0) | (index == levels) | (index >= 2 * levels)
        high = (index == levels - 1) | (index >= 2 * levels - 1)
        return jnp.where(low, 0.0, near(mid, -1, axis)) + jnp.where(high, 0.0, near(mid, 1, axis))

    row_weights = [weigh(t_row[i], above_below(t_row[i], layer, 0)) for i in (0, 1)]
    col_weights = [weigh(t, above_below(t, lane, 1)) for t in (tleft, tright)]
    each("wait_recv", ("row", "pack"))
    for i, dx in enumerate((-1, 1)):
        halo = row_recv[i]
        for dy in (-1, 0, 1):
            d = DIRS.index((dx, dy))
            val = halo
            if dy != 0:
                val = jnp.where(edge_col == (0 if dy < 0 else cols - 1), 0.0, near(halo, dy, 1))
            part = jnp.sum(row_weights[i][1 if dy != 0 else 0] * val, axis=0, keepdims=True)
            coefs[d] = coefs[d] + jnp.where(row_id == (0 if dx < 0 else rows - 1), part, 0.0)
    for i, dy in enumerate((-1, 1)):
        at = beside(dy)
        for dx in (-1, 0, 1):
            d = DIRS.index((dx, dy))
            part = jnp.sum(col_weights[i][1 if dx != 0 else 0] * at[dx], axis=1, keepdims=True)
            coefs[d] = coefs[d] + jnp.where(col_id == (0 if dy < 0 else cols - 1), part, 0.0)
    for d in range(8):
        k_send[d] = coefs[d]
    kleft, kright = pack(coefs, 0, blank, blank)
    kp_send[0] = kleft
    kp_send[1] = kright
    each("start", ("coefpack", "coef"))

    def extend(j, mine, recv, packs_ref, index, place):
        for tile, dx in enumerate((-1, 0, 1)):
            here = mine if dx == 0 else recv[0 if dx < 0 else 1, index]
            from_right = packs_ref[DIRS.index((dx, 1)) - 2]
            from_left = packs_ref[DIRS.index((dx, -1)) - 2]
            halo = jnp.where(lane < REACH, roll(from_right, -place, 1), 0.0)
            halo = jnp.where(lane >= 128 - REACH, roll(from_left, 128 - REACH - place, 1), halo)
            ext[j, tile * rows:(tile + 1) * rows, :cols] = here
            ext[j, tile * rows:(tile + 1) * rows, cols:] = halo

    each("wait_recv", ("field",))
    for j in range(FIELDS):
        extend(j, f_send[j], f_recv, p_recv, j, 2 * levels + REACH * j)
    each("wait_recv", ("coefpack", "coef"))
    for d in range(8):
        extend(FIELDS + d, k_send[d], k_recv, kp_recv, d, REACH * d)

    def coef(dx, dy):
        return ext[FIELDS + DIRS.index((dx, dy))]

    def forth(q):
        spread = [ext[0] * q, ext[1] * q]
        surface = [ext[4] * spread[0], ext[4] * spread[1]]
        for dx in (-1, 0, 1):
            moved = [near(s, dx, 0) for s in spread]
            for dy in (-1, 0, 1):
                if (dx, dy) == (0, 0):
                    continue
                share = cross_share * dx * dy
                for c in range(2):
                    val = moved[c] if share == 0 else moved[c] + share * moved[1 - c]
                    surface[c] = surface[c] + coef(dx, dy) * near(val, dy, 1)
        return surface

    def back(q, surface):
        traction = [ext[2] * s for s in surface]
        basal = [ext[4] * t for t in traction]
        for dx in (-1, 0, 1):
            part = [None, None]
            for dy in (-1, 0, 1):
                if (dx, dy) == (0, 0):
                    continue
                share = cross_share * dx * dy
                for c in range(2):
                    val = traction[c] if share == 0 else traction[c] + share * traction[1 - c]
                    val = near(coef(-dx, -dy) * val, dy, 1)
                    part[c] = val if part[c] is None else part[c] + val
            basal = [basal[c] + near(part[c], dx, 0) for c in range(2)]
        return ext[0] * basal[0] + ext[1] * basal[1] + regularize(q)

    def regularize(q):
        around = near(q, 1, 0) + near(q, -1, 0) + near(q, 1, 1) + near(q, -1, 1)
        return reg_gamma * (q + reg_smooth * (4.0 * q - around))

    def hessian(q):
        return back(q, forth(q))

    def mine(x):
        return x[rows:2 * rows, :cols]

    warm = ext[5]
    image = hessian(warm)
    r0 = ext[6] - image
    p0 = ext[3] * r0
    w0 = hessian(p0)
    y0 = ext[3] * w0
    surface = forth(y0)
    curve0 = mine(ext[2]) * (mine(surface[0]) * mine(surface[0]) + mine(surface[1]) * mine(surface[1])) + mine(y0 * regularize(y0))
    full_y0 = y0
    r0, p0, w0, y0 = mine(r0), mine(p0), mine(w0), mine(y0)

    def total(x):
        return jnp.sum(jnp.sum(x, axis=0, keepdims=True), axis=1, keepdims=True)

    one_lane = lax.broadcasted_iota(jnp.int32, (1, 128), 1)
    sums = jnp.zeros((1, 128), jnp.float32)
    for j, val in enumerate((r0 * p0, p0 * w0, w0 * y0, curve0)):
        sums = jnp.where(one_lane == j, total(val), sums)
    red[...] = sums

    def to_peer(peer):
        return pltpu.make_async_remote_copy(
            src_ref=red, dst_ref=slots.at[me], send_sem=r_send, recv_sem=r_recv,
            device_id=peer, device_id_type=LOGICAL,
        )

    everybody = pltpu.make_async_remote_copy(
        src_ref=slots.at[pl.ds(0, n - 1)], dst_ref=slots.at[pl.ds(0, n - 1)], send_sem=r_send, recv_sem=r_recv,
        device_id=me, device_id_type=LOGICAL,
    )

    def send(j, c):
        peer = lax.rem(2 * n - 1 - me + j, n)

        @pl.when(peer != me)
        def _():
            to_peer(peer).start()
        return c

    pl.semaphore_wait(all_in, ny - 1)
    lax.fori_loop(0, n, send, 0, unroll=8)
    u0 = mine(back(full_y0, surface))
    each("wait_send", [name for name, _ in kinds])
    everybody.wait_recv()
    slots[me] = sums
    everyone = jnp.sum(slots[...], axis=0)

    def pick(j):
        return jnp.sum(jnp.where(one_lane == j, everyone, 0.0), axis=1, keepdims=True)

    rz0, pw, wy, yu = pick(0), pick(1), pick(2), pick(3)
    a0 = rz0 / pw
    rz1 = a0 * a0 * wy - rz0
    beta = rz1 / rz0
    more = 1.0 + beta
    curve = more * (more * pw - 2.0 * a0 * wy) + a0 * a0 * yu
    a1 = rz1 / curve
    out_ref[0] = warm_ref[...] + (a0 * p0 + a1 * (more * p0 - a0 * y0))
    out_ref[1] = grad_ref[...] + (-mine(image) - a0 * w0 - a1 * (more * w0 - a0 * u0))
    everybody.wait_send()


def solution(mesh):
    nx, ny = mesh.shape["gx"], mesh.shape["gy"]
    n = nx * ny

    def on_device(gradient, warm_start, viscosity, friction_coef, slide_dir, obs_weight, ice_mask, grounded):
        levels, rows, cols = viscosity.shape
        vmem = pl.BlockSpec(memory_space=pltpu.VMEM)
        f32 = lambda *shape: pltpu.VMEM(shape, jnp.float32)
        flat = (gradient, warm_start, viscosity, friction_coef, slide_dir, obs_weight, ice_mask, grounded)
        out = pl.pallas_call(
            functools.partial(kernel, nx, ny),
            out_shape=f32(2, rows, cols),
            in_specs=[pl.BlockSpec(memory_space=pl.ANY)] * 8,
            out_specs=vmem,
            scratch_shapes=[
                *(pltpu.VMEM(a.shape, a.dtype) for a in flat),
                f32(levels, rows, cols), f32(levels, rows, cols),
                f32(levels, rows, cols), f32(levels, rows, cols),
                f32(levels + 2, rows, cols), f32(levels + 2, rows, cols),
                f32(2, 2 * levels, cols), f32(2, 2 * levels, cols), f32(2, 2 * levels, cols),
                f32(FIELDS, rows, cols), f32(2, FIELDS, rows, cols),
                f32(2, rows, 128), f32(6, rows, 128),
                f32(8, rows, cols), f32(2, 8, rows, cols),
                f32(2, rows, 128), f32(6, rows, 128),
                f32(FIELDS + 8, 3 * rows, cols + 128),
                f32(1, 128), f32(n, 1, 128),
                pltpu.SemaphoreType.DMA((8,)),
                pltpu.SemaphoreType.DMA((24,)), pltpu.SemaphoreType.DMA((24,)),
                pltpu.SemaphoreType.DMA, pltpu.SemaphoreType.DMA,
                pltpu.SemaphoreType.REGULAR,
            ],
            compiler_params=pltpu.CompilerParams(collective_id=0, has_side_effects=True),
        )(*flat)
        return out[0], out[1]

    flat = P("gx", "gy")
    deep = P(None, "gx", "gy")
    return jax.shard_map(
        on_device,
        mesh=mesh,
        in_specs=(flat, flat, deep, flat, deep, flat, flat, flat),
        out_specs=(flat, flat),
        check_vma=False,
    )
```

```python
import functools

import jax
import jax.numpy as jnp
from jax import lax
from jax.experimental import pallas as pl
from jax.experimental.pallas import tpu as pltpu
from jax.sharding import PartitionSpec as P

vert_coupling = 128.0
sink_rate = 0.0625
bed_drag = 0.5
offset_weight = 0.0019
cross_share = 0.5
reg_gamma = 0.02
reg_smooth = 1.0
diag_scale = 0.003

MESH = pl.DeviceIdType.MESH
LOGICAL = pl.DeviceIdType.LOGICAL
REACH = 6
DIRS = [(-1, 0), (1, 0), (0, -1), (0, 1), (-1, -1), (-1, 1), (1, -1), (1, 1)]
OPPOSITE = [1, 0, 3, 2, 7, 6, 5, 4]
BASE = 6


def roll(x, shift, axis):
    size = x.shape[axis]
    if isinstance(shift, int):
        shift = shift % size
        if shift == 0:
            return x
    return pltpu.roll(x, shift, axis)


def near(x, step, axis):
    return roll(x, -step, axis)


def kernel(
    nx, ny,
    grad_in, warm_in, visc_in, fric_in, slide_in, obs_in, ice_in, ground_in,
    out_ref,
    grad_ref, warm_ref, visc_ref, fric_ref, slide_ref, obs_ref, ice_ref, ground_ref,
    up, down, bot, gbot, top, gtop,
    vx, upx, downx, bx, gx, tx, hx,
    e_send, ef, a_send, a_recv, c_send, c_recv, k_send, k_recv,
    pk_send, pk_recv, px_recv, q_send, q_recv,
    ext, red, slots,
    load_sem, s_send, s_recv, r_send, r_recv, all_in,
):
    levels, rows, cols = visc_ref.shape
    n = nx * ny
    ix, iy = lax.axis_index("gx"), lax.axis_index("gy")
    me = ix * ny + iy

    loads = [
        pltpu.make_async_copy(src, dst, load_sem.at[j])
        for j, (src, dst) in enumerate((
            (visc_in, visc_ref), (fric_in, fric_ref), (ground_in, ground_ref), (ice_in, ice_ref),
            (slide_in, slide_ref), (obs_in, obs_ref), (warm_in, warm_ref), (grad_in, grad_ref),
        ))
    ]

    def exists(d):
        dx, dy = DIRS[d]
        x, y = ix + dx, iy + dy
        return (x >= 0) & (x < nx) & (y >= 0) & (y < ny)

    barrier = pltpu.get_barrier_semaphore()

    def greet(x, y):
        pl.semaphore_signal(barrier, inc=1, device_id=(x, y), device_id_type=MESH)

    for load in loads:
        load.start()
    expected = nx - 1 + ny - 1
    for d in range(4, 8):
        expected = expected + exists(d).astype(jnp.int32)

        @pl.when(exists(d))
        def _():
            greet(ix + DIRS[d][0], iy + DIRS[d][1])
    for k in range(1, nx):
        greet(lax.rem(ix + k, nx), iy)
    for k in range(1, ny):
        greet(ix, lax.rem(iy + k, ny))

    def copy(src, dst, d, sem):
        dx, dy = DIRS[d]
        return pltpu.make_async_remote_copy(
            src_ref=src, dst_ref=dst,
            send_sem=s_send.at[sem + d], recv_sem=s_recv.at[sem + OPPOSITE[d]],
            device_id=(jnp.clip(ix + dx, 0, nx - 1), jnp.clip(iy + dy, 0, ny - 1)),
            device_id_type=MESH,
        )

    def message(d, what):
        o = OPPOSITE[d]
        dx, dy = DIRS[d]
        side = 0 if dy < 0 else 1

        def part(k):
            return pl.ds(0 if dx < 0 else rows - k, k)

        return {
            "pack": lambda: copy(pk_send.at[side], pk_recv.at[o - 2], d, 0),
            "visc": lambda: copy(visc_ref.at[:, part(1), :], vx.at[:, part(1), pl.ds(0, cols)], d, 0),
            "late": lambda: copy(q_send.at[side], q_recv.at[o - 2], d, 8),
            "edge": lambda: copy(e_send.at[:, part(1), :], ef.at[:, part(1), :], d, 8),
            "side": lambda: copy(pk_send.at[:, 0], px_recv.at[o], d, 16),
            "wide": lambda: copy(a_send.at[:, part(REACH), :], a_recv.at[o, :, part(REACH), :], d, 18),
            "less": lambda: copy(c_send.at[:, part(REACH - 2), :], c_recv.at[o, :, part(REACH - 2), :], d, 20),
            "coef": lambda: copy(k_send.at[:, part(REACH - 1), :], k_recv.at[o, :, part(REACH - 1), :], d, 22),
        }[what]()

    beside_x, others = (0, 1), range(2, 8)
    kinds = (
        ("pack", others), ("visc", beside_x), ("edge", beside_x), ("side", beside_x), ("wide", beside_x), ("less", beside_x),
        ("late", others), ("coef", beside_x),
    )

    def each(action, names):
        for name, towards in kinds:
            if name not in names:
                continue
            for d in towards:
                @pl.when(exists(d))
                def _():
                    if action == "wait_recv":
                        message(OPPOSITE[d], name).wait_recv()
                    elif action == "wait_send":
                        message(d, name).wait_send()
                    else:
                        message(d, name).start()

    def fill(ref, value=0.0):
        ref[...] = jnp.full(ref.shape, value, jnp.float32)

    for d in range(8):
        @pl.when(jnp.logical_not(exists(d)))
        def _():
            if d < 2:
                row = pl.ds(rows - 1 if d == 0 else 0, 1)
                fill(vx.at[:, row, pl.ds(0, cols)], 1.0)
                fill(ef.at[:, row, :])
                for ref in (px_recv, a_recv, c_recv, k_recv):
                    fill(ref.at[d])
            else:
                fill(pk_recv.at[d - 2, 0])
                fill(pk_recv.at[d - 2, 1], 1.0)
                fill(pk_recv.at[d - 2, 2])
                fill(q_recv.at[d - 2])

    for load in loads:
        load.wait()

    ice = ice_ref[...].astype(jnp.float32)
    ground = ground_ref[...].astype(jnp.float32)
    fric = fric_ref[...]
    friction = ground * fric
    base = ice * ground * fric
    inverse = 1.0 / (reg_gamma * (1.0 + 4.0 * reg_smooth) + diag_scale * base * fric)
    watch = ice * jnp.sqrt(obs_ref[...])
    turned = base * (0.5 ** 0.5)
    sum_src = turned * (slide_ref[0] + slide_ref[1])
    dif_src = turned * (slide_ref[0] - slide_ref[1])
    lane = lax.broadcasted_iota(jnp.int32, (rows, 128), 1)
    prow = lax.broadcasted_iota(jnp.int32, (rows, 128), 0)

    def factor(v, up, down, drag):
        def eliminate(i, carry):
            e, f = carry
            k = levels - 2 - i
            v_low, v_up = v[i], v[i + 1]
            link = (vert_coupling * 0.5) * (v_low + v_up)
            ratio = link / (link + e)
            up[i] = ratio
            e = sink_rate * v_up + e * ratio
            w_low, w_up = v[k], v[k + 1]
            link = (vert_coupling * 0.5) * (w_low + w_up)
            ratio = link / (link + f)
            down[k] = ratio
            f = sink_rate * w_low + f * ratio
            return e, f

        e = sink_rate * v[0] + drag
        f = sink_rate * v[levels - 1]
        e, f = lax.fori_loop(0, levels - 1, eliminate, (e, f), unroll=True)
        return e, f + drag

    def layer(z):
        return pl.ds(z * rows, rows)

    def put(ref, z, val):
        for c in range(val.shape[1] // 128):
            ref[c, layer(z), :] = val[:, c * 128:(c + 1) * 128]

    def get(ref, z):
        return jnp.concatenate([ref[c, layer(z), :] for c in range(ref.shape[0])], axis=1)

    e, f = factor(visc_ref, up, down, bed_drag * friction)
    zero = jnp.zeros((rows, cols), jnp.float32)
    for ref in (top, gtop):
        put(ref, 0, zero)
        put(ref, levels + 1, zero)

    blank = jnp.zeros((rows, 128), jnp.float32)
    half = levels // 2
    left, right = blank, blank
    near_left, near_right = [blank + 1.0] * 2, [blank + 1.0] * 2
    b, t = (0.25 * offset_weight) / f, watch / e
    for z in range(levels):
        k = levels - 1 - z
        v = visc_ref[z]
        g, h = v * b, visc_ref[k] * t
        put(bot, z, b)
        put(gbot, z, g)
        put(top, k + 1, t)
        put(gtop, k + 1, h)
        for place, val in ((z, b), (levels + z, g), (2 * levels + k, h), (3 * levels + k, t)):
            left = jnp.where(lane == place, roll(val[:, :128], place, 1), left)
            right = jnp.where(lane == place, roll(val[:, cols - 128:], place + 1, 1), right)
        place = REACH * (z % half)
        here = (lane >= place) & (lane < place + REACH)
        near_left[z // half] = jnp.where(here, roll(v[:, :128], place, 1), near_left[z // half])
        near_right[z // half] = jnp.where(here, roll(v[:, cols - 128:], place + REACH, 1), near_right[z // half])
        if z < levels - 1:
            t = t * up[k - 1]
            b = b * down[z]
    through = t

    def pack(fields, place, left, right):
        for val in fields:
            here = (lane >= place) & (lane < place + REACH)
            left = jnp.where(here, roll(val[:, :128], place, 1), left)
            right = jnp.where(here, roll(val[:, cols - 128:], place - (128 - REACH), 1), right)
            place += REACH
        return left, right

    for j, val in enumerate((sum_src, dif_src, warm_ref[...])):
        a_send[j] = val
    for j, val in enumerate((inverse, grad_ref[...])):
        c_send[j] = val
    k_send[0] = through
    for j, val in enumerate((friction, watch)):
        e_send[j] = val
    fields = pack((sum_src, dif_src, warm_ref[...], inverse, grad_ref[...], through, friction, watch), 0, blank, blank)
    folded = (prow == 1) | (prow == 2)
    for side, strip, sight in ((0, left, near_left), (1, right, near_right)):
        pk_send[side, 0] = strip
        pk_send[side, 1] = jnp.where(folded, roll(sight[1], 2, 0), sight[0])
        pk_send[side, 2] = fields[side]

    pl.semaphore_wait(barrier, expected)
    each("start", ("pack", "visc", "edge", "side", "wide", "less"))
    for k in range(1, ny):
        pl.semaphore_signal(all_in, inc=1, device_id=(ix, lax.rem(iy + k, ny)), device_id_type=MESH)

    def weigh(mid, out):
        return 2.0 * mid + out, mid + (2.0 / 3.0) * out

    def gather(z, acc):
        acc = list(acc)
        for ref, other in ((bot, gtop), (gbot, top)):
            straight, slant = weigh(get(other, z + 1), get(other, z) + get(other, z + 2))
            mid = get(ref, z)
            for dy, val in ((-1, near(mid, -1, 1)), (0, mid), (1, near(mid, 1, 1))):
                for dx in (-1, 0, 1):
                    if (dx, dy) != (0, 0):
                        d = DIRS.index((dx, dy))
                        weight = slant if dx * dy != 0 else straight
                        acc[d] = acc[d] + (weight if dx == 0 else near(weight, -dx, 0)) * val
        return tuple(acc)

    row_id = lax.broadcasted_iota(jnp.int32, (rows, cols), 0)
    col_id = lax.broadcasted_iota(jnp.int32, (rows, cols), 1)
    coefs = list(lax.fori_loop(0, levels, gather, (zero,) * 8, unroll=8))
    for d, (dx, dy) in enumerate(DIRS):
        if dx != 0:
            coefs[d] = jnp.where(row_id == (0 if dx < 0 else rows - 1), 0.0, near(coefs[d], dx, 0))
        if dy != 0:
            coefs[d] = jnp.where(col_id == (0 if dy < 0 else cols - 1), 0.0, coefs[d])
        k_send[1 + d] = coefs[d]
    q_send[0], q_send[1] = pack(coefs, 0, blank, blank)
    each("start", ("late", "coef"))

    def pick(packs, dx, dy):
        return packs[DIRS.index((dx, dy)) - 2]

    def corner(which, dy):
        flat = [pk_recv[DIRS.index((dx, dy)) - 2, which] for dx in (-1, 1)]
        return jnp.where((prow == 0) | (prow == 2), flat[1], flat[0])

    inner = (lane >= 32) & (lane < 96)
    after = lane < 64

    def frame(which):
        sides = [pk_recv[DIRS.index((0, dy)) - 2, which] for dy in (1, -1)]
        corners = [corner(which, dy) for dy in (1, -1)]

        def at(place):
            ahead = jnp.where(inner, roll(corners[0], 64 - place, 1), roll(sides[0], -place, 1))
            behind = jnp.where(inner, roll(corners[1], 64 - REACH - place, 1), roll(sides[1], -REACH - place, 1))
            return jnp.where(inner, jnp.where(lane < 64, behind, ahead), jnp.where(after, ahead, behind))
        return at

    each("wait_recv", ("pack", "visc", "edge"))
    sight = frame(1)
    for z in range(half):
        both = sight(REACH * z)
        vx[z, :, cols:] = both
        vx[z + half, :, cols:] = near(both, 2, 0)
    known = frame(2)

    def strip_field(j, place):
        return jnp.concatenate([ef[j], known(place)], axis=1)

    e, f = factor(vx, upx, downx, bed_drag * strip_field(0, 6 * REACH))
    b, t = (0.25 * offset_weight) / f, strip_field(1, 7 * REACH) / e
    for z in range(levels):
        k = levels - 1 - z
        put(bx, z, b)
        put(gx, z, vx[z] * b)
        put(tx, k, t)
        put(hx, k, vx[k] * t)
        if z < levels - 1:
            t = t * upx[k - 1]
            b = b * downx[z]

    main, halo = range(cols // 128), range(cols // 128, cols // 128 + 1)

    def strip(ref, row, tiles, first=0):
        return jnp.concatenate([ref[c, pl.ds(first * rows + row, levels, stride=rows), :] for c in tiles], axis=1)

    def own_row(row):
        return [strip(bot, row, main), strip(gbot, row, main), strip(gtop, row, main, 1), strip(top, row, main, 1)]

    def far_row(row):
        return [strip(ref, row, main) for ref in (bx, gx, hx, tx)]

    def side_row(row):
        return [strip(ref, row, halo) for ref in (bx, gx, hx, tx)]

    def corner_row(row):
        return [roll(val, 64, 1) for val in side_row(row)]

    def level_weights(mid):
        index = lax.broadcasted_iota(jnp.int32, mid.shape, 0)
        out = jnp.where(index == 0, 0.0, near(mid, -1, 0)) + jnp.where(index == levels - 1, 0.0, near(mid, 1, 0))
        return weigh(mid, out)

    def across(here, there):
        by_b, by_g = level_weights(here[2]), level_weights(here[3])
        width = here[0].shape[1]
        at = lax.broadcasted_iota(jnp.int32, (1, width), 1)
        parts = []
        for dy in (-1, 0, 1):
            which = 1 if dy != 0 else 0
            part = jnp.sum(by_b[which] * near(there[0], dy, 1) + by_g[which] * near(there[1], dy, 1), axis=0, keepdims=True)
            parts.append(part if dy == 0 else jnp.where(at == (0 if dy < 0 else width - 1), 0.0, part))
        return parts

    def join(first, second):
        return [jnp.concatenate(pair, axis=1) for pair in zip(first, second)]

    last = rows - 1
    lines = {}
    pieces = ((own_row(last), far_row(0)), (side_row(last), corner_row(0)))
    lines[2 * rows - 1] = join(*[across(low, high) for low, high in pieces])
    lines[2 * rows] = join(*[across(high, low) for low, high in pieces])
    pieces = ((far_row(last), own_row(0)), (corner_row(last), side_row(0)))
    lines[rows - 1] = join(*[across(low, high) for low, high in pieces])
    lines[rows] = join(*[across(high, low) for low, high in pieces])

    each("wait_recv", ("side",))
    tall_lane = lax.broadcasted_iota(jnp.int32, (3 * rows, 128), 1)

    def column(mine_side, dy):
        if dy == 0:
            tiles = [px_recv[0, mine_side], pk_send[mine_side, 0], px_recv[1, mine_side]]
        else:
            tiles = [pk_recv[DIRS.index((dx, dy)) - 2, 0] for dx in (-1, 0, 1)]
        return jnp.concatenate(tiles, axis=0)

    level_of = lax.rem(tall_lane, levels)

    def beside(here, there):
        out = jnp.where(level_of == 0, 0.0, near(here, -1, 1)) + jnp.where(level_of == levels - 1, 0.0, near(here, 1, 1))
        straight, slant = [jnp.where(tall_lane < 2 * levels, near(w, 2 * levels, 1), 0.0) for w in weigh(here, out)]
        return [jnp.sum((straight if dx == 0 else slant) * near(there, dx, 0), axis=1, keepdims=True) for dx in (-1, 0, 1)]

    west, east = (column(1, -1), column(0, 0)), (column(1, 0), column(0, 1))
    posts = {
        1: ((cols + 127, beside(west[0], west[1])), (cols - 1, beside(east[0], east[1]))),
        -1: ((0, beside(west[1], west[0])), (cols, beside(east[1], east[0]))),
    }

    def extend(j, mine, recv, packs, place):
        for tile, dx in enumerate((-1, 0, 1)):
            here = mine if dx == 0 else recv(0 if dx < 0 else 1)
            from_right, from_left = packs(dx, 1), packs(dx, -1)
            side = jnp.where(lane < REACH, roll(from_right, -place, 1), 0.0)
            side = jnp.where(lane >= 128 - REACH, roll(from_left, 128 - REACH - place, 1), side)
            ext[j, tile * rows:(tile + 1) * rows, :cols] = here
            ext[j, tile * rows:(tile + 1) * rows, cols:] = side

    def early(dx, dy):
        return pk_recv[DIRS.index((dx, dy)) - 2, 2]

    def late(dx, dy):
        return q_recv[DIRS.index((dx, dy)) - 2]

    each("wait_recv", ("wide", "less"))
    for j in range(3):
        extend(j, a_send[j], lambda i: a_recv[i, j], early, REACH * j)
    for j in range(2):
        extend(3 + j, c_send[j], lambda i: c_recv[i, j], early, REACH * (3 + j))
    each("wait_recv", ("late", "coef"))
    extend(5, k_send[0], lambda i: k_recv[i, 0], early, REACH * 5)
    wide_col = lax.broadcasted_iota(jnp.int32, (3 * rows, cols + 128), 1)
    for d, (dx, dy) in enumerate(DIRS):
        extend(BASE + d, k_send[1 + d], lambda i: k_recv[i, 1 + d], late, REACH * d)
        if dy != 0:
            whole = ext[BASE + d]
            for spot, parts in posts[dy]:
                whole = whole + jnp.where(wide_col == spot, parts[dx + 1], 0.0)
            ext[BASE + d] = whole
        if dx != 0:
            for row in ((rows - 1, 2 * rows - 1) if dx > 0 else (rows, 2 * rows)):
                ext[BASE + d, row:row + 1, :] = ext[BASE + d, row:row + 1, :] + lines[row][dy + 1]

    def coef(dx, dy):
        return ext[BASE + DIRS.index((dx, dy))]

    shares = (1.0 + cross_share, 1.0 - cross_share)

    def forth(q):
        surface = []
        for c in range(2):
            spread = ext[c] * q
            total = ext[5] * spread
            sums = {1: None, -1: None}
            for dy in (-1, 0, 1):
                turned = near(spread, dy, 1)
                for dx in (-1, 0, 1):
                    if (dx, dy) == (0, 0):
                        continue
                    val = coef(dx, dy) * near(turned, dx, 0)
                    if dx * dy == 0:
                        total = total + val
                    else:
                        sums[dx * dy] = val if sums[dx * dy] is None else sums[dx * dy] + val
            surface.append(total + shares[c] * sums[1] + shares[1 - c] * sums[-1])
        return surface

    def back(q, surface):
        result = regularize(q)
        for c in range(2):
            pull = surface[c]
            scaled = {0: pull, 1: shares[c] * pull, -1: shares[1 - c] * pull}
            basal = ext[5] * pull
            for dy in (-1, 0, 1):
                part = None
                for dx in (-1, 0, 1):
                    if (dx, dy) == (0, 0):
                        continue
                    val = near(coef(-dx, -dy) * scaled[dx * dy], dx, 0)
                    part = val if part is None else part + val
                basal = basal + near(part, dy, 1)
            result = result + ext[c] * basal
        return result

    def regularize(q):
        around = near(q, 1, 0) + near(q, -1, 0) + near(q, 1, 1) + near(q, -1, 1)
        return reg_gamma * (q + reg_smooth * (4.0 * q - around))

    def hessian(q):
        return back(q, forth(q))

    def mine(x):
        return x[rows:2 * rows, :cols]

    image = hessian(ext[2])
    r0 = ext[4] - image
    p0 = ext[3] * r0
    w0 = hessian(p0)
    y0 = ext[3] * w0
    surface = forth(y0)
    curve0 = mine(surface[0]) * mine(surface[0]) + mine(surface[1]) * mine(surface[1]) + mine(y0 * regularize(y0))
    full_y0 = y0
    r0, p0, w0, y0 = mine(r0), mine(p0), mine(w0), mine(y0)

    def total(x):
        return jnp.sum(jnp.sum(x, axis=0, keepdims=True), axis=1, keepdims=True)

    one_lane = lax.broadcasted_iota(jnp.int32, (1, 128), 1)
    sums = jnp.zeros((1, 128), jnp.float32)
    for j, val in enumerate((r0 * p0, p0 * w0, w0 * y0, curve0)):
        sums = jnp.where(one_lane == j, total(val), sums)
    red[...] = sums

    def to_peer(peer):
        return pltpu.make_async_remote_copy(
            src_ref=red, dst_ref=slots.at[me], send_sem=r_send, recv_sem=r_recv,
            device_id=peer, device_id_type=LOGICAL,
        )

    everybody = pltpu.make_async_remote_copy(
        src_ref=slots.at[pl.ds(0, n - 1)], dst_ref=slots.at[pl.ds(0, n - 1)], send_sem=r_send, recv_sem=r_recv,
        device_id=me, device_id_type=LOGICAL,
    )

    def send(j, c):
        peer = lax.rem(2 * n - 1 - me + j, n)

        @pl.when(peer != me)
        def _():
            to_peer(peer).start()
        return c

    pl.semaphore_wait(all_in, ny - 1)
    lax.fori_loop(0, n, send, 0, unroll=8)
    u0 = mine(back(full_y0, surface))
    each("wait_send", [name for name, _ in kinds])
    everybody.wait_recv()
    slots[me] = sums
    everyone = jnp.sum(slots[...], axis=0)

    def value(j):
        return jnp.sum(jnp.where(one_lane == j, everyone, 0.0), axis=1, keepdims=True)

    rz0, pw, wy, yu = value(0), value(1), value(2), value(3)
    a0 = rz0 / pw
    rz1 = a0 * a0 * wy - rz0
    beta = rz1 / rz0
    more = 1.0 + beta
    curve = more * (more * pw - 2.0 * a0 * wy) + a0 * a0 * yu
    a1 = rz1 / curve
    out_ref[0] = warm_ref[...] + (a0 * p0 + a1 * (more * p0 - a0 * y0))
    out_ref[1] = grad_ref[...] + (-mine(image) - a0 * w0 - a1 * (more * w0 - a0 * u0))
    everybody.wait_send()


def solution(mesh):
    nx, ny = mesh.shape["gx"], mesh.shape["gy"]
    n = nx * ny

    def on_device(gradient, warm_start, viscosity, friction_coef, slide_dir, obs_weight, ice_mask, grounded):
        levels, rows, cols = viscosity.shape
        vmem = pl.BlockSpec(memory_space=pltpu.VMEM)
        f32 = lambda *shape: pltpu.VMEM(shape, jnp.float32)
        flat = (gradient, warm_start, viscosity, friction_coef, slide_dir, obs_weight, ice_mask, grounded)
        out = pl.pallas_call(
            functools.partial(kernel, nx, ny),
            out_shape=f32(2, rows, cols),
            in_specs=[pl.BlockSpec(memory_space=pl.ANY)] * 8,
            out_specs=vmem,
            scratch_shapes=[
                *(pltpu.VMEM(a.shape, a.dtype) for a in flat),
                f32(levels, rows, cols), f32(levels, rows, cols),
                *(f32(cols // 128, levels * rows, 128) for _ in range(2)),
                *(f32(cols // 128, (levels + 2) * rows, 128) for _ in range(2)),
                *(f32(levels, rows, cols + 128) for _ in range(3)),
                *(f32(cols // 128 + 1, levels * rows, 128) for _ in range(4)),
                f32(2, rows, cols), f32(2, rows, cols),
                f32(3, rows, cols), f32(2, 3, rows, cols),
                f32(2, rows, cols), f32(2, 2, rows, cols),
                f32(9, rows, cols), f32(2, 9, rows, cols),
                f32(2, 3, rows, 128), f32(6, 3, rows, 128), f32(2, 2, rows, 128),
                f32(2, rows, 128), f32(6, rows, 128),
                f32(BASE + 8, 3 * rows, cols + 128),
                f32(1, 128), f32(n, 1, 128),
                pltpu.SemaphoreType.DMA((8,)),
                pltpu.SemaphoreType.DMA((24,)), pltpu.SemaphoreType.DMA((24,)),
                pltpu.SemaphoreType.DMA, pltpu.SemaphoreType.DMA,
                pltpu.SemaphoreType.REGULAR,
            ],
            compiler_params=pltpu.CompilerParams(collective_id=0, has_side_effects=True),
        )(*flat)
        return out[0], out[1]

    flat = P("gx", "gy")
    deep = P(None, "gx", "gy")
    return jax.shard_map(
        on_device,
        mesh=mesh,
        in_specs=(flat, flat, deep, flat, deep, flat, flat, flat),
        out_specs=(flat, flat),
        check_vma=False,
    )
```

```python
import functools

import jax
import jax.numpy as jnp
from jax import lax
from jax.experimental import pallas as pl
from jax.experimental.pallas import tpu as pltpu
from jax.sharding import PartitionSpec as P

vert_coupling = 128.0
sink_rate = 0.0625
bed_drag = 0.5
offset_weight = 0.0019
cross_share = 0.5
reg_gamma = 0.02
reg_smooth = 1.0
diag_scale = 0.003

MESH = pl.DeviceIdType.MESH
LOGICAL = pl.DeviceIdType.LOGICAL
REACH = 6
DIRS = [(-1, 0), (1, 0), (0, -1), (0, 1), (-1, -1), (-1, 1), (1, -1), (1, 1)]
OPPOSITE = [1, 0, 3, 2, 7, 6, 5, 4]
BASE = 6


def roll(x, shift, axis):
    size = x.shape[axis]
    if isinstance(shift, int):
        shift = shift % size
        if shift == 0:
            return x
    return pltpu.roll(x, shift, axis)


def near(x, step, axis):
    return roll(x, -step, axis)


def kernel(
    nx, ny,
    grad_in, warm_in, visc_in, fric_in, slide_in, obs_in, ice_in, ground_in,
    out_ref,
    grad_ref, warm_ref, visc_ref, fric_ref, slide_ref, obs_ref, ice_ref, ground_ref,
    up, down, bot, gbot, top, gtop,
    vx, upx, downx, bx, gx, tx, hx,
    e_send, ef, a_send, a_recv, c_send, c_recv, k_send, k_recv,
    q_send, q_recv, d_send, d_recv, px_send, px_recv,
    ext, red, slots,
    load_sem, s_send, s_recv, r_send, r_recv, entered,
):
    levels, rows, cols = visc_ref.shape
    n = nx * ny
    ix, iy = lax.axis_index("gx"), lax.axis_index("gy")
    me = ix * ny + iy

    loads = [
        pltpu.make_async_copy(src, dst, load_sem.at[j])
        for j, (src, dst) in enumerate((
            (visc_in, visc_ref), (fric_in, fric_ref), (ground_in, ground_ref), (ice_in, ice_ref),
            (slide_in, slide_ref), (obs_in, obs_ref), (warm_in, warm_ref), (grad_in, grad_ref),
        ))
    ]

    def exists(d):
        dx, dy = DIRS[d]
        x, y = ix + dx, iy + dy
        return (x >= 0) & (x < nx) & (y >= 0) & (y < ny)

    barrier = pltpu.get_barrier_semaphore()

    def greet(x, y):
        pl.semaphore_signal(barrier, inc=1, device_id=(x, y), device_id_type=MESH)

    for load in loads:
        load.start()
    expected = ny - 1
    for d in (0, 1):
        expected = expected + exists(d).astype(jnp.int32)

        @pl.when(exists(d))
        def _():
            greet(ix + DIRS[d][0], iy)
    for k in range(1, ny):
        greet(ix, lax.rem(iy + k, ny))
    rounds = entered.shape[0]

    def herald(r):
        for side, step in ((1, -(2 ** r)), (0, 2 ** r)):
            @pl.when((ix + step >= 0) & (ix + step < nx))
            def _():
                pl.semaphore_signal(entered.at[r, side], inc=1, device_id=(ix + step, iy), device_id_type=MESH)

    def hear(r):
        for side, step in ((0, -(2 ** r)), (1, 2 ** r)):
            @pl.when((ix + step >= 0) & (ix + step < nx))
            def _():
                pl.semaphore_wait(entered.at[r, side], 1)

    def copy(src, dst, d, sem):
        dx, dy = DIRS[d]
        return pltpu.make_async_remote_copy(
            src_ref=src, dst_ref=dst,
            send_sem=s_send.at[sem + d], recv_sem=s_recv.at[sem + OPPOSITE[d]],
            device_id=(jnp.clip(ix + dx, 0, nx - 1), jnp.clip(iy + dy, 0, ny - 1)),
            device_id_type=MESH,
        )

    def message(d, what):
        o = OPPOSITE[d]
        dx, dy = DIRS[d]
        side = 0 if dy < 0 else 1

        def part(k):
            return pl.ds(0 if dx < 0 else rows - k, k)

        return {
            "visc": lambda: copy(visc_ref.at[:, part(1), :], vx.at[:, part(1), :], d, 0),
            "slant": lambda: copy(d_send.at[d - 4], d_recv.at[o - 4], d, 0),
            "edge": lambda: copy(e_send.at[:, part(1), :], ef.at[:, part(1), :], d, 8),
            "late": lambda: copy(q_send.at[side], q_recv.at[o - 2], d, 0),
            "side": lambda: copy(px_send.at[:, part(REACH), :], px_recv.at[o, :, part(REACH), :], d, 10),
            "wide": lambda: copy(a_send.at[:, part(REACH), :], a_recv.at[o, :, part(REACH), :], d, 12),
            "less": lambda: copy(c_send.at[:, part(REACH - 2), :], c_recv.at[o, :, part(REACH - 2), :], d, 14),
            "coef": lambda: copy(k_send.at[:, part(REACH - 1), :], k_recv.at[o, :, part(REACH - 1), :], d, 16),
        }[what]()

    along_x, along_y, aslant = (0, 1), (2, 3), (4, 5, 6, 7)
    for_x, for_y = ("visc", "edge", "wide", "less", "side", "coef"), ("late",)

    def each(action, names, towards):
        for name in names:
            for d in towards:
                @pl.when(exists(d))
                def _():
                    if action == "wait_recv":
                        message(OPPOSITE[d], name).wait_recv()
                    elif action == "wait_send":
                        message(d, name).wait_send()
                    else:
                        message(d, name).start()

    def fill(ref, value=0.0):
        ref[...] = jnp.full(ref.shape, value, jnp.float32)

    for d in range(8):
        @pl.when(jnp.logical_not(exists(d)))
        def _():
            if d < 2:
                row = pl.ds(rows - 1 if d == 0 else 0, 1)
                fill(vx.at[:, row, :], 1.0)
                fill(ef.at[:, row, :])
                for ref in (px_recv, a_recv, c_recv, k_recv):
                    fill(ref.at[d])
            elif d < 4:
                fill(q_recv.at[d - 2])
            else:
                fill(d_recv.at[d - 4])

    for load in loads:
        load.wait()

    ice = ice_ref[...].astype(jnp.float32)
    ground = ground_ref[...].astype(jnp.float32)
    fric = fric_ref[...]
    friction = ground * fric
    base = ice * ground * fric
    inverse = 1.0 / (reg_gamma * (1.0 + 4.0 * reg_smooth) + diag_scale * base * fric)
    watch = ice * jnp.sqrt(obs_ref[...])
    turned = base * (0.5 ** 0.5)
    sum_src = turned * (slide_ref[0] + slide_ref[1])
    dif_src = turned * (slide_ref[0] - slide_ref[1])
    lane = lax.broadcasted_iota(jnp.int32, (rows, 128), 1)
    prow = lax.broadcasted_iota(jnp.int32, (rows, 128), 0)

    def factor(v, up, down, drag):
        def eliminate(i, carry):
            e, f = carry
            k = levels - 2 - i
            v_low, v_up = v[i], v[i + 1]
            link = (vert_coupling * 0.5) * (v_low + v_up)
            ratio = link / (link + e)
            up[i] = ratio
            e = sink_rate * v_up + e * ratio
            w_low, w_up = v[k], v[k + 1]
            link = (vert_coupling * 0.5) * (w_low + w_up)
            ratio = link / (link + f)
            down[k] = ratio
            f = sink_rate * w_low + f * ratio
            return e, f

        e = sink_rate * v[0] + drag
        f = sink_rate * v[levels - 1]
        e, f = lax.fori_loop(0, levels - 1, eliminate, (e, f), unroll=True)
        return e, f + drag

    def layer(z):
        return pl.ds(z * rows, rows)

    def put(ref, z, val):
        for c in range(val.shape[1] // 128):
            ref[c, layer(z), :] = val[:, c * 128:(c + 1) * 128]

    def get(ref, z):
        return jnp.concatenate([ref[c, layer(z), :] for c in range(ref.shape[0])], axis=1)

    zero = jnp.zeros((rows, cols), jnp.float32)
    for ref in (top, gtop):
        put(ref, 0, zero)
        put(ref, levels + 1, zero)

    blank = jnp.zeros((rows, 128), jnp.float32)
    def rim(val):
        return jnp.where(lane < 64, val[:, :128], val[:, cols - 128:])

    def within(place, width):
        start = place % 128
        return (lane >= start) & (lane < start + width)

    def pack(fields, place, left, right):
        for val in fields:
            moved = roll(rim(val), place, 1)
            left = jnp.where(within(place, REACH), moved, left)
            right = jnp.where(within(place - REACH, REACH), moved, right)
            place += REACH
        return left, right

    for j, val in enumerate((sum_src, dif_src, warm_ref[...])):
        a_send[j] = val
    for j, val in enumerate((inverse, grad_ref[...])):
        c_send[j] = val
    for j, val in enumerate((friction, watch)):
        e_send[j] = val
    e, f = factor(visc_ref, up, down, bed_drag * friction)
    pl.semaphore_wait(barrier, expected)
    herald(0)
    each("start", ("visc", "edge", "wide", "less"), along_x)
    left, right = blank, blank
    b, t = (0.25 * offset_weight) / f, watch / e
    for z in range(levels):
        k = levels - 1 - z
        v = visc_ref[z]
        g, h = v * b, visc_ref[k] * t
        put(bot, z, b)
        put(gbot, z, g)
        put(top, k + 1, t)
        put(gtop, k + 1, h)
        for place, val in ((z, b), (levels + z, g), (2 * levels + k, h), (3 * levels + k, t)):
            moved = roll(rim(val), place, 1)
            left = jnp.where(lane == place, moved, left)
            right = jnp.where(lane == (place - 1) % 128, moved, right)
        if z < levels - 1:
            t = t * up[k - 1]
            b = b * down[z]
    through = t
    right = roll(right, 1, 1)
    k_send[0] = through
    px_send[0], px_send[1] = left, right
    each("start", ("side",), along_x)
    spans = [(q, tile) for q in range(4) for tile in range(levels // rows)]

    def spot(q, tile):
        return tile * (128 * rows // levels) + REACH * q

    for side in (0, 1):
        q_send[side, 1] = (left, right)[side]
        d_send[side, 1] = (left, right)[side]
        d_send[2 + side, 1] = (left, right)[side]
    for j, row in enumerate((0, rows - 1)):
        corner = [blank, blank]
        for q, tile in spans:
            ref, first = ((bot, 0), (gbot, 0), (gtop, 1), (top, 1))[q]
            span = pl.ds((first + tile * rows) * rows + row, rows, stride=rows)
            place = spot(q, tile)
            moved = roll(jnp.where(lane < 64, ref[0, span, :], ref[cols // 128 - 1, span, :]), place, 1)
            corner[0] = jnp.where(within(place, REACH), moved, corner[0])
            corner[1] = jnp.where(within(place - REACH, REACH), moved, corner[1])
        for side in (0, 1):
            q_send[side, 2 + j] = corner[side]
            d_send[2 * j + side, 2] = corner[side]
    fields = pack((sum_src, dif_src, warm_ref[...], inverse, grad_ref[...], through), 0, blank, blank)

    def weigh(mid, out):
        return 2.0 * mid + out, mid + (2.0 / 3.0) * out

    def gather(z, acc):
        acc = list(acc)
        for ref, other in ((bot, gtop), (gbot, top)):
            straight, slant = weigh(get(other, z + 1), get(other, z) + get(other, z + 2))
            mid = get(ref, z)
            for dy, val in ((-1, near(mid, -1, 1)), (0, mid), (1, near(mid, 1, 1))):
                for dx in (-1, 0, 1):
                    if (dx, dy) != (0, 0):
                        d = DIRS.index((dx, dy))
                        weight = slant if dx * dy != 0 else straight
                        acc[d] = acc[d] + (weight if dx == 0 else near(weight, -dx, 0)) * val
        return tuple(acc)

    row_id = lax.broadcasted_iota(jnp.int32, (rows, cols), 0)
    col_id = lax.broadcasted_iota(jnp.int32, (rows, cols), 1)
    coefs = list(lax.fori_loop(0, levels, gather, (zero,) * 8, unroll=16))
    for d, (dx, dy) in enumerate(DIRS):
        if dx != 0:
            coefs[d] = jnp.where(row_id == (0 if dx < 0 else rows - 1), 0.0, near(coefs[d], dx, 0))
        if dy != 0:
            coefs[d] = jnp.where(col_id == (0 if dy < 0 else cols - 1), 0.0, coefs[d])
        k_send[1 + d] = coefs[d]
    fields = pack(coefs, REACH * BASE, *fields)
    for side in (0, 1):
        q_send[side, 0] = fields[side]
        for j in (0, 1):
            d_send[2 * j + side, 0] = fields[side]
    each("start", ("late",), along_y)
    hear(0)
    each("start", ("slant",), aslant)
    each("start", ("coef",), along_x)
    if rounds > 1:
        herald(1)

    def respond(v, up, down, drag, sight, refs):
        e, f = factor(v, up, down, drag)
        b, t = (0.25 * offset_weight) / f, sight / e
        for z in range(levels):
            k = levels - 1 - z
            put(refs[0], z, b)
            put(refs[1], z, v[z] * b)
            put(refs[2], k, v[k] * t)
            put(refs[3], k, t)
            if z < levels - 1:
                t = t * up[k - 1]
                b = b * down[z]

    far = (bx, gx, hx, tx)
    def strip(ref, row, first=0):
        return jnp.concatenate(
            [ref[c, pl.ds(first * rows + row, levels, stride=rows), :] for c in range(ref.shape[0])], axis=1
        )

    def own_row(row):
        return [strip(bot, row), strip(gbot, row), strip(gtop, row, 1), strip(top, row, 1)]

    def far_row(row):
        return [strip(ref, row) for ref in far]

    phase = lax.rem(lane, 128 * rows // levels)

    def unfold(ahead, behind):
        mixed = []
        for odd in (0, REACH):
            first = (phase >= odd) & (phase < odd + REACH) | (phase >= odd + 2 * REACH) & (phase < odd + 3 * REACH)
            mixed.append(jnp.where(first, ahead, behind))
        return [
            jnp.concatenate([roll(mixed[q % 2], -spot(q, tile), 1) for tile in range(levels // rows)], axis=0)
            for q in range(4)
        ]

    def side_row(row):
        return unfold(*[q_recv[y, 2 if row == 0 else 3] for y in (1, 0)])

    def corner_row(row):
        dx = 1 if row == 0 else -1
        return unfold(*[d_recv[DIRS.index((dx, dy)) - 4, 2] for dy in (1, -1)])

    def level_weights(mid):
        index = lax.broadcasted_iota(jnp.int32, mid.shape, 0)
        out = jnp.where(index == 0, 0.0, near(mid, -1, 0)) + jnp.where(index == levels - 1, 0.0, near(mid, 1, 0))
        return weigh(mid, out)

    def ready(vals):
        moved = [[near(val, dy, 1) for val in vals[:2]] for dy in (-1, 0, 1)]
        return level_weights(vals[2]), level_weights(vals[3]), moved

    def across(here, there):
        width = there[2][0][0].shape[1]
        at = lax.broadcasted_iota(jnp.int32, (1, width), 1)
        parts = []
        for dy in (-1, 0, 1):
            which = 1 if dy != 0 else 0
            by_b, by_g = there[2][dy + 1]
            part = jnp.sum(here[0][which] * by_b + here[1][which] * by_g, axis=0, keepdims=True)
            parts.append(part if dy == 0 else jnp.where(at == (0 if dy < 0 else width - 1), 0.0, part))
        return parts

    last = rows - 1
    low, high = ready(own_row(0)), ready(own_row(last))
    each("wait_recv", ("visc", "edge"), along_x)
    respond(vx, upx, downx, bed_drag * ef[0], ef[1], far)
    below, above = ready(far_row(last)), ready(far_row(0))
    lines = {
        2 * rows - 1: across(high, above), 2 * rows: across(above, high),
        rows - 1: across(below, low), rows: across(low, below),
    }
    each("wait_recv", ("side", "wide", "less"), along_x)
    each("wait_recv", ("late",), along_y)
    low, high = ready(side_row(0)), ready(side_row(last))
    level_of = lax.rem(lane, levels)

    def beyond(dx, dy, which):
        return q_recv[0 if dy < 0 else 1, which] if dx == 0 else d_recv[DIRS.index((dx, dy)) - 4, which]

    def column(mine_side):
        return [px_recv[0, mine_side], q_send[mine_side, 1], px_recv[1, mine_side]]

    def slope(here):
        out = jnp.where(level_of == 0, 0.0, near(here, -1, 1)) + jnp.where(level_of == levels - 1, 0.0, near(here, 1, 1))
        return [jnp.where(lane < 2 * levels, near(w, 2 * levels, 1), 0.0) for w in weigh(here, out)]

    def stack(tiles):
        return jnp.concatenate(tiles, axis=0)

    def beside(slopes, there):
        straight, slant = [stack([each_slope[i] for each_slope in slopes]) for i in (0, 1)]
        there = stack(there)
        return [jnp.sum((straight if dx == 0 else slant) * near(there, dx, 0), axis=1, keepdims=True) for dx in (-1, 0, 1)]

    inside = [[slope(tile) for tile in column(side)] for side in (0, 1)]
    outside = [slope(beyond(0, dy, 1)) for dy in (-1, 1)]

    even = within(0, REACH)
    for j in range(2, BASE + 8, 2):
        even = even | within(REACH * j, REACH)
    odd = within(REACH, REACH)
    for j in range(3, BASE + 8, 2):
        odd = odd | within(REACH * j, REACH)

    def mix(dx):
        return [jnp.where(first, beyond(dx, 1, 0), beyond(dx, -1, 0)) for first in (even, odd)]

    def extend(j, mine, recv):
        for tile, here in enumerate((recv(0), mine, recv(1))):
            ext[j, tile * rows:(tile + 1) * rows, :cols] = here

    kept = (lane < REACH) | (lane >= 128 - REACH)

    def frame(j, tile, mixed):
        ext[j, tile * rows:(tile + 1) * rows, cols:] = jnp.where(kept, roll(mixed[j % 2], -REACH * j, 1), 0.0)

    mixed = mix(0)
    for j in range(3):
        extend(j, a_send[j], lambda i: a_recv[i, j])
    for j in range(2):
        extend(3 + j, c_send[j], lambda i: c_recv[i, j])
    for j in range(BASE + 8):
        frame(j, 1, mixed)

    each("wait_recv", ("slant",), aslant)
    below, above = ready(corner_row(last)), ready(corner_row(0))
    edges = {
        2 * rows - 1: across(high, above), 2 * rows: across(above, high),
        rows - 1: across(below, low), rows: across(low, below),
    }
    for row in lines:
        lines[row] = [jnp.concatenate(pair, axis=1) for pair in zip(lines[row], edges[row])]
    posts = {1: [], -1: []}
    for side, dy in ((0, -1), (1, 1)):
        tiles = [beyond(dx, dy, 1) for dx in (-1, 0, 1)]
        slopes = [slope(tiles[0]), outside[side], slope(tiles[2])]
        posts[dy].append((cols - 1 if dy > 0 else 0, beside(inside[side], tiles)))
        posts[-dy].append((cols if dy > 0 else cols + 127, beside(slopes, column(side))))
    for tile, dx in ((0, -1), (2, 1)):
        mixed = mix(dx)
        for j in range(BASE + 8):
            frame(j, tile, mixed)
    each("wait_recv", ("coef",), along_x)
    extend(5, k_send[0], lambda i: k_recv[i, 0])
    wide_col = lax.broadcasted_iota(jnp.int32, (3 * rows, cols + 128), 1)
    for d, (dx, dy) in enumerate(DIRS):
        extend(BASE + d, k_send[1 + d], lambda i: k_recv[i, 1 + d])
        if dy != 0:
            whole = ext[BASE + d]
            for spot, parts in posts[dy]:
                whole = whole + jnp.where(wide_col == spot, parts[dx + 1], 0.0)
            ext[BASE + d] = whole
        if dx != 0:
            for row in ((rows - 1, 2 * rows - 1) if dx > 0 else (rows, 2 * rows)):
                ext[BASE + d, row:row + 1, :] = ext[BASE + d, row:row + 1, :] + lines[row][dy + 1]

    def coef(dx, dy):
        return ext[BASE + DIRS.index((dx, dy))]

    shares = (1.0 + cross_share, 1.0 - cross_share)

    def forth(q):
        surface = []
        for c in range(2):
            spread = ext[c] * q
            total = ext[5] * spread
            sums = {1: None, -1: None}
            for dy in (-1, 0, 1):
                turned = near(spread, dy, 1)
                for dx in (-1, 0, 1):
                    if (dx, dy) == (0, 0):
                        continue
                    val = coef(dx, dy) * near(turned, dx, 0)
                    if dx * dy == 0:
                        total = total + val
                    else:
                        sums[dx * dy] = val if sums[dx * dy] is None else sums[dx * dy] + val
            surface.append(total + shares[c] * sums[1] + shares[1 - c] * sums[-1])
        return surface

    def back(q, surface):
        result = regularize(q)
        for c in range(2):
            pull = surface[c]
            scaled = {0: pull, 1: shares[c] * pull, -1: shares[1 - c] * pull}
            basal = ext[5] * pull
            for dy in (-1, 0, 1):
                part = None
                for dx in (-1, 0, 1):
                    if (dx, dy) == (0, 0):
                        continue
                    val = near(coef(-dx, -dy) * scaled[dx * dy], dx, 0)
                    part = val if part is None else part + val
                basal = basal + near(part, dy, 1)
            result = result + ext[c] * basal
        return result

    def regularize(q):
        around = near(q, 1, 0) + near(q, -1, 0) + near(q, 1, 1) + near(q, -1, 1)
        return reg_gamma * (q + reg_smooth * (4.0 * q - around))

    def hessian(q):
        return back(q, forth(q))

    def mine(x):
        return x[rows:2 * rows, :cols]

    image = hessian(ext[2])
    r0 = ext[4] - image
    p0 = ext[3] * r0
    w0 = hessian(p0)
    y0 = ext[3] * w0
    surface = forth(y0)
    curve0 = mine(surface[0]) * mine(surface[0]) + mine(surface[1]) * mine(surface[1]) + mine(y0 * regularize(y0))
    full_y0 = y0
    r0, p0, w0, y0 = mine(r0), mine(p0), mine(w0), mine(y0)

    def total(x):
        return jnp.sum(jnp.sum(x, axis=0, keepdims=True), axis=1, keepdims=True)

    one_lane = lax.broadcasted_iota(jnp.int32, (1, 128), 1)
    sums = jnp.zeros((1, 128), jnp.float32)
    for j, val in enumerate((r0 * p0, p0 * w0, w0 * y0, curve0)):
        sums = jnp.where(one_lane == j, total(val), sums)
    red[...] = sums

    def to_peer(peer):
        return pltpu.make_async_remote_copy(
            src_ref=red, dst_ref=slots.at[me], send_sem=r_send, recv_sem=r_recv,
            device_id=peer, device_id_type=LOGICAL,
        )

    everybody = pltpu.make_async_remote_copy(
        src_ref=slots.at[pl.ds(0, n - 1)], dst_ref=slots.at[pl.ds(0, n - 1)], send_sem=r_send, recv_sem=r_recv,
        device_id=me, device_id_type=LOGICAL,
    )

    def send(j, c):
        peer = lax.rem(2 * n - 1 - me + j, n)

        @pl.when(peer != me)
        def _():
            to_peer(peer).start()
        return c

    for r in range(1, rounds):
        hear(r)
        if r + 1 < rounds:
            herald(r + 1)
    lax.fori_loop(0, n, send, 0, unroll=8)
    u0 = mine(back(full_y0, surface))
    each("wait_send", for_x, along_x)
    each("wait_send", for_y, along_y)
    each("wait_send", ("slant",), aslant)
    everybody.wait_recv()
    slots[me] = sums
    everyone = jnp.sum(slots[...], axis=0)

    def value(j):
        return jnp.sum(jnp.where(one_lane == j, everyone, 0.0), axis=1, keepdims=True)

    rz0, pw, wy, yu = value(0), value(1), value(2), value(3)
    a0 = rz0 / pw
    rz1 = a0 * a0 * wy - rz0
    beta = rz1 / rz0
    more = 1.0 + beta
    curve = more * (more * pw - 2.0 * a0 * wy) + a0 * a0 * yu
    a1 = rz1 / curve
    out_ref[0] = warm_ref[...] + (a0 * p0 + a1 * (more * p0 - a0 * y0))
    out_ref[1] = grad_ref[...] + (-mine(image) - a0 * w0 - a1 * (more * w0 - a0 * u0))
    everybody.wait_send()


def solution(mesh):
    nx, ny = mesh.shape["gx"], mesh.shape["gy"]
    n = nx * ny

    def on_device(gradient, warm_start, viscosity, friction_coef, slide_dir, obs_weight, ice_mask, grounded):
        levels, rows, cols = viscosity.shape
        vmem = pl.BlockSpec(memory_space=pltpu.VMEM)
        f32 = lambda *shape: pltpu.VMEM(shape, jnp.float32)
        flat = (gradient, warm_start, viscosity, friction_coef, slide_dir, obs_weight, ice_mask, grounded)
        out = pl.pallas_call(
            functools.partial(kernel, nx, ny),
            out_shape=f32(2, rows, cols),
            in_specs=[pl.BlockSpec(memory_space=pl.ANY)] * 8,
            out_specs=vmem,
            scratch_shapes=[
                *(pltpu.VMEM(a.shape, a.dtype) for a in flat),
                f32(levels, rows, cols), f32(levels, rows, cols),
                *(f32(cols // 128, levels * rows, 128) for _ in range(2)),
                *(f32(cols // 128, (levels + 2) * rows, 128) for _ in range(2)),
                *(f32(levels, rows, cols) for _ in range(3)),
                *(f32(cols // 128, levels * rows, 128) for _ in range(4)),
                f32(2, rows, cols), f32(2, rows, cols),
                f32(3, rows, cols), f32(2, 3, rows, cols),
                f32(2, rows, cols), f32(2, 2, rows, cols),
                f32(9, rows, cols), f32(2, 9, rows, cols),
                f32(2, 4, rows, 128), f32(2, 4, rows, 128),
                f32(4, 3, rows, 128), f32(4, 3, rows, 128), f32(2, rows, 128), f32(2, 2, rows, 128),
                f32(BASE + 8, 3 * rows, cols + 128),
                f32(1, 128), f32(n, 1, 128),
                pltpu.SemaphoreType.DMA((8,)),
                pltpu.SemaphoreType.DMA((18,)), pltpu.SemaphoreType.DMA((18,)),
                pltpu.SemaphoreType.DMA, pltpu.SemaphoreType.DMA,
                pltpu.SemaphoreType.REGULAR((max(1, (nx - 1).bit_length()), 2)),
            ],
            compiler_params=pltpu.CompilerParams(collective_id=0, has_side_effects=True),
        )(*flat)
        return out[0], out[1]

    flat = P("gx", "gy")
    deep = P(None, "gx", "gy")
    return jax.shard_map(
        on_device,
        mesh=mesh,
        in_specs=(flat, flat, deep, flat, deep, flat, flat, flat),
        out_specs=(flat, flat),
        check_vma=False,
    )
```

```python
import functools

import jax
import jax.numpy as jnp
from jax import lax
from jax.experimental import pallas as pl
from jax.experimental.pallas import tpu as pltpu
from jax.sharding import PartitionSpec as P

vert_coupling = 128.0
sink_rate = 0.0625
bed_drag = 0.5
offset_weight = 0.0019
cross_share = 0.5
reg_gamma = 0.02
reg_smooth = 1.0
diag_scale = 0.003

MESH = pl.DeviceIdType.MESH
LOGICAL = pl.DeviceIdType.LOGICAL
REACH = 6
DIRS = [(-1, 0), (1, 0), (0, -1), (0, 1), (-1, -1), (-1, 1), (1, -1), (1, 1)]
OPPOSITE = [1, 0, 3, 2, 7, 6, 5, 4]
BASE = 6


def roll(x, shift, axis):
    size = x.shape[axis]
    if isinstance(shift, int):
        shift = shift % size
        if shift == 0:
            return x
    return pltpu.roll(x, shift, axis)


def near(x, step, axis):
    return roll(x, -step, axis)


def kernel(
    nx, ny,
    grad_in, warm_in, visc_in, fric_in, slide_in, obs_in, ice_in, ground_in,
    out_ref,
    grad_ref, warm_ref, visc_ref, fric_ref, slide_ref, obs_ref, ice_ref, ground_ref,
    up, down, bot, gbot, top, gtop,
    vx, upx, downx, bx, gx, tx, hx,
    e_send, ef, a_send, a_recv, c_send, c_recv, k_send, k_recv,
    q_send, q_recv, d_send, d_recv, px_send, px_recv,
    ext, red, slots,
    load_sem, s_send, s_recv, r_send, r_recv, entered,
):
    levels, rows, cols = visc_ref.shape
    n = nx * ny
    ix, iy = lax.axis_index("gx"), lax.axis_index("gy")
    me = ix * ny + iy

    loads = [
        pltpu.make_async_copy(src, dst, load_sem.at[min(j, 1)])
        for j, (src, dst) in enumerate((
            (visc_in, visc_ref), (fric_in, fric_ref), (ground_in, ground_ref), (ice_in, ice_ref),
            (slide_in, slide_ref), (obs_in, obs_ref), (warm_in, warm_ref), (grad_in, grad_ref),
        ))
    ]

    def exists(d):
        dx, dy = DIRS[d]
        x, y = ix + dx, iy + dy
        return (x >= 0) & (x < nx) & (y >= 0) & (y < ny)

    barrier = pltpu.get_barrier_semaphore()

    def greet(x, y):
        pl.semaphore_signal(barrier, inc=1, device_id=(x, y), device_id_type=MESH)

    for load in loads:
        load.start()
    expected = ny - 1
    for d in (0, 1):
        expected = expected + exists(d).astype(jnp.int32)

        @pl.when(exists(d))
        def _():
            greet(ix + DIRS[d][0], iy)
    for k in range(1, ny):
        greet(ix, lax.rem(iy + k, ny))
    rounds = entered.shape[0]

    def herald(r):
        for side, step in ((1, -(2 ** r)), (0, 2 ** r)):
            @pl.when((ix + step >= 0) & (ix + step < nx))
            def _():
                pl.semaphore_signal(entered.at[r, side], inc=1, device_id=(ix + step, iy), device_id_type=MESH)

    def hear(r):
        for side, step in ((0, -(2 ** r)), (1, 2 ** r)):
            @pl.when((ix + step >= 0) & (ix + step < nx))
            def _():
                pl.semaphore_wait(entered.at[r, side], 1)

    def copy(src, dst, d, sem):
        dx, dy = DIRS[d]
        return pltpu.make_async_remote_copy(
            src_ref=src, dst_ref=dst,
            send_sem=s_send.at[d], recv_sem=s_recv.at[sem + OPPOSITE[d]],
            device_id=(jnp.clip(ix + dx, 0, nx - 1), jnp.clip(iy + dy, 0, ny - 1)),
            device_id_type=MESH,
        )

    def message(d, what):
        o = OPPOSITE[d]
        dx, dy = DIRS[d]
        side = 0 if dy < 0 else 1

        def part(k):
            return pl.ds(0 if dx < 0 else rows - k, k)

        return {
            "visc": lambda: copy(visc_ref.at[:, part(1), :], vx.at[:, part(1), :], d, 0),
            "slant": lambda: copy(d_send.at[d - 4], d_recv.at[o - 4], d, 0),
            "edge": lambda: copy(e_send.at[:, part(1), :], ef.at[:, part(1), :], d, 8),
            "late": lambda: copy(q_send.at[side], q_recv.at[o - 2], d, 0),
            "side": lambda: copy(px_send.at[:, part(REACH), :], px_recv.at[o, :, part(REACH), :], d, 10),
            "wide": lambda: copy(a_send.at[:, part(REACH), :], a_recv.at[o, :, part(REACH), :], d, 12),
            "less": lambda: copy(c_send.at[:, part(REACH - 2), :], c_recv.at[o, :, part(REACH - 2), :], d, 14),
            "coef": lambda: copy(k_send.at[:, part(REACH - 1), :], k_recv.at[o, :, part(REACH - 1), :], d, 16),
        }[what]()

    along_x, along_y, aslant = (0, 1), (2, 3), (4, 5, 6, 7)
    for_x, for_y = ("visc", "edge", "wide", "less", "side", "coef"), ("late",)

    def each(action, names, towards):
        for name in names:
            for d in towards:
                @pl.when(exists(d))
                def _():
                    if action == "wait_recv":
                        message(OPPOSITE[d], name).wait_recv()
                    elif action == "wait_send":
                        message(d, name).wait_send()
                    else:
                        message(d, name).start()

    def fill(ref, value=0.0):
        ref[...] = jnp.full(ref.shape, value, jnp.float32)

    for d in range(8):
        @pl.when(jnp.logical_not(exists(d)))
        def _():
            if d < 2:
                row = pl.ds(rows - 1 if d == 0 else 0, 1)
                fill(vx.at[:, row, :], 1.0)
                fill(ef.at[:, row, :])
                for ref in (px_recv, a_recv, c_recv, k_recv):
                    fill(ref.at[d])
            elif d < 4:
                fill(q_recv.at[d - 2])
            else:
                fill(d_recv.at[d - 4])

    loads[0].wait()
    pltpu.make_async_copy(visc_in.at[pl.ds(0, 8)], up.at[pl.ds(0, 8)], load_sem.at[1]).wait()

    ice = ice_ref[...].astype(jnp.float32)
    ground = ground_ref[...].astype(jnp.float32)
    fric = fric_ref[...]
    friction = ground * fric
    base = ice * ground * fric
    inverse = 1.0 / (reg_gamma * (1.0 + 4.0 * reg_smooth) + diag_scale * base * fric)
    watch = ice * jnp.sqrt(obs_ref[...])
    turned = base * (0.5 ** 0.5)
    sum_src = turned * (slide_ref[0] + slide_ref[1])
    dif_src = turned * (slide_ref[0] - slide_ref[1])
    lane = lax.broadcasted_iota(jnp.int32, (rows, 128), 1)
    prow = lax.broadcasted_iota(jnp.int32, (rows, 128), 0)

    def factor(v, up, down, drag):
        def eliminate(i, carry):
            e, f = carry
            k = levels - 2 - i
            v_low, v_up = v[i], v[i + 1]
            link = (vert_coupling * 0.5) * (v_low + v_up)
            ratio = link / (link + e)
            up[i] = ratio
            e = sink_rate * v_up + e * ratio
            w_low, w_up = v[k], v[k + 1]
            link = (vert_coupling * 0.5) * (w_low + w_up)
            ratio = link / (link + f)
            down[k] = ratio
            f = sink_rate * w_low + f * ratio
            return e, f

        e = sink_rate * v[0] + drag
        f = sink_rate * v[levels - 1]
        e, f = lax.fori_loop(0, levels - 1, eliminate, (e, f), unroll=True)
        return e, f + drag

    def layer(z):
        return pl.ds(z * rows, rows)

    def put(ref, z, val):
        for c in range(val.shape[1] // 128):
            ref[c, layer(z), :] = val[:, c * 128:(c + 1) * 128]

    def get(ref, z):
        return jnp.concatenate([ref[c, layer(z), :] for c in range(ref.shape[0])], axis=1)

    zero = jnp.zeros((rows, cols), jnp.float32)
    for ref in (top, gtop):
        put(ref, 0, zero)
        put(ref, levels + 1, zero)

    blank = jnp.zeros((rows, 128), jnp.float32)
    def rim(val):
        return jnp.where(lane < 64, val[:, :128], val[:, cols - 128:])

    def within(place, width):
        start = place % 128
        return (lane >= start) & (lane < start + width)

    def pack(fields, place, left, right):
        for val in fields:
            moved = roll(rim(val), place, 1)
            left = jnp.where(within(place, REACH), moved, left)
            right = jnp.where(within(place - REACH, REACH), moved, right)
            place += REACH
        return left, right

    for j, val in enumerate((sum_src, dif_src, warm_ref[...])):
        a_send[j] = val
    for j, val in enumerate((inverse, grad_ref[...])):
        c_send[j] = val
    for j, val in enumerate((friction, watch)):
        e_send[j] = val
    e, f = factor(visc_ref, up, down, bed_drag * friction)
    pl.semaphore_wait(barrier, expected)
    herald(0)
    each("start", ("visc", "edge", "wide", "less"), along_x)
    left, right = blank, blank
    b, t = (0.25 * offset_weight) / f, watch / e
    for z in range(levels):
        k = levels - 1 - z
        v = visc_ref[z]
        g, h = v * b, visc_ref[k] * t
        put(bot, z, b)
        put(gbot, z, g)
        put(top, k + 1, t)
        put(gtop, k + 1, h)
        for place, val in ((z, b), (levels + z, g), (2 * levels + k, h), (3 * levels + k, t)):
            moved = roll(rim(val), place, 1)
            left = jnp.where(lane == place, moved, left)
            right = jnp.where(lane == (place - 1) % 128, moved, right)
        if z < levels - 1:
            t = t * up[k - 1]
            b = b * down[z]
    through = t
    right = roll(right, 1, 1)
    k_send[0] = through
    px_send[0], px_send[1] = left, right
    each("start", ("side",), along_x)
    spans = [(q, tile) for q in range(4) for tile in range(levels // rows)]

    def spot(q, tile):
        return tile * (128 * rows // levels) + REACH * q

    for side in (0, 1):
        q_send[side, 1] = (left, right)[side]
        d_send[side, 1] = (left, right)[side]
        d_send[2 + side, 1] = (left, right)[side]
    for j, row in enumerate((0, rows - 1)):
        corner = [blank, blank]
        for q, tile in spans:
            ref, first = ((bot, 0), (gbot, 0), (gtop, 1), (top, 1))[q]
            span = pl.ds((first + tile * rows) * rows + row, rows, stride=rows)
            place = spot(q, tile)
            moved = roll(jnp.where(lane < 64, ref[0, span, :], ref[cols // 128 - 1, span, :]), place, 1)
            corner[0] = jnp.where(within(place, REACH), moved, corner[0])
            corner[1] = jnp.where(within(place - REACH, REACH), moved, corner[1])
        for side in (0, 1):
            q_send[side, 2 + j] = corner[side]
            d_send[2 * j + side, 2] = corner[side]
    fields = pack((sum_src, dif_src, warm_ref[...], inverse, grad_ref[...], through), 0, blank, blank)

    def weigh(mid, out):
        return 2.0 * mid + out, mid + (2.0 / 3.0) * out

    def gather(z, acc):
        acc = list(acc)
        for ref, other in ((bot, gtop), (gbot, top)):
            straight, slant = weigh(get(other, z + 1), get(other, z) + get(other, z + 2))
            mid = get(ref, z)
            for dy, val in ((-1, near(mid, -1, 1)), (0, mid), (1, near(mid, 1, 1))):
                for dx in (-1, 0, 1):
                    if (dx, dy) != (0, 0):
                        d = DIRS.index((dx, dy))
                        weight = slant if dx * dy != 0 else straight
                        acc[d] = acc[d] + (weight if dx == 0 else near(weight, -dx, 0)) * val
        return tuple(acc)

    row_id = lax.broadcasted_iota(jnp.int32, (rows, cols), 0)
    col_id = lax.broadcasted_iota(jnp.int32, (rows, cols), 1)
    coefs = list(lax.fori_loop(0, levels, gather, (zero,) * 8, unroll=16))
    for d, (dx, dy) in enumerate(DIRS):
        if dx != 0:
            coefs[d] = jnp.where(row_id == (0 if dx < 0 else rows - 1), 0.0, near(coefs[d], dx, 0))
        if dy != 0:
            coefs[d] = jnp.where(col_id == (0 if dy < 0 else cols - 1), 0.0, coefs[d])
        k_send[1 + d] = coefs[d]
    fields = pack(coefs, REACH * BASE, *fields)
    for side in (0, 1):
        q_send[side, 0] = fields[side]
        for j in (0, 1):
            d_send[2 * j + side, 0] = fields[side]
    each("start", ("late",), along_y)
    hear(0)
    each("start", ("slant",), aslant)
    each("start", ("coef",), along_x)
    if rounds > 1:
        herald(1)

    def respond(v, up, down, drag, sight, refs):
        e, f = factor(v, up, down, drag)
        b, t = (0.25 * offset_weight) / f, sight / e
        for z in range(levels):
            k = levels - 1 - z
            put(refs[0], z, b)
            put(refs[1], z, v[z] * b)
            put(refs[2], k, v[k] * t)
            put(refs[3], k, t)
            if z < levels - 1:
                t = t * up[k - 1]
                b = b * down[z]

    far = (bx, gx, hx, tx)
    def strip(ref, row, first=0):
        return jnp.concatenate(
            [ref[c, pl.ds(first * rows + row, levels, stride=rows), :] for c in range(ref.shape[0])], axis=1
        )

    def own_row(row):
        return [strip(bot, row), strip(gbot, row), strip(gtop, row, 1), strip(top, row, 1)]

    def far_row(row):
        return [strip(ref, row) for ref in far]

    phase = lax.rem(lane, 128 * rows // levels)

    def unfold(ahead, behind):
        mixed = []
        for odd in (0, REACH):
            first = (phase >= odd) & (phase < odd + REACH) | (phase >= odd + 2 * REACH) & (phase < odd + 3 * REACH)
            mixed.append(jnp.where(first, ahead, behind))
        return [
            jnp.concatenate([roll(mixed[q % 2], -spot(q, tile), 1) for tile in range(levels // rows)], axis=0)
            for q in range(4)
        ]

    def side_row(row):
        return unfold(*[q_recv[y, 2 if row == 0 else 3] for y in (1, 0)])

    def corner_row(row):
        dx = 1 if row == 0 else -1
        return unfold(*[d_recv[DIRS.index((dx, dy)) - 4, 2] for dy in (1, -1)])

    def level_weights(mid):
        index = lax.broadcasted_iota(jnp.int32, mid.shape, 0)
        out = jnp.where(index == 0, 0.0, near(mid, -1, 0)) + jnp.where(index == levels - 1, 0.0, near(mid, 1, 0))
        return weigh(mid, out)

    def ready(vals):
        moved = [[near(val, dy, 1) for val in vals[:2]] for dy in (-1, 0, 1)]
        return level_weights(vals[2]), level_weights(vals[3]), moved

    def across(here, there):
        width = there[2][0][0].shape[1]
        at = lax.broadcasted_iota(jnp.int32, (1, width), 1)
        parts = []
        for dy in (-1, 0, 1):
            which = 1 if dy != 0 else 0
            by_b, by_g = there[2][dy + 1]
            part = jnp.sum(here[0][which] * by_b + here[1][which] * by_g, axis=0, keepdims=True)
            parts.append(part if dy == 0 else jnp.where(at == (0 if dy < 0 else width - 1), 0.0, part))
        return parts

    last = rows - 1
    low, high = ready(own_row(0)), ready(own_row(last))
    each("wait_recv", ("visc", "edge"), along_x)
    respond(vx, upx, downx, bed_drag * ef[0], ef[1], far)
    below, above = ready(far_row(last)), ready(far_row(0))
    lines = {
        2 * rows - 1: across(high, above), 2 * rows: across(above, high),
        rows - 1: across(below, low), rows: across(low, below),
    }
    each("wait_recv", ("side", "wide", "less"), along_x)
    each("wait_recv", ("late",), along_y)
    low, high = ready(side_row(0)), ready(side_row(last))
    level_of = lax.rem(lane, levels)

    def beyond(dx, dy, which):
        return q_recv[0 if dy < 0 else 1, which] if dx == 0 else d_recv[DIRS.index((dx, dy)) - 4, which]

    def column(mine_side):
        return [px_recv[0, mine_side], q_send[mine_side, 1], px_recv[1, mine_side]]

    def slope(here):
        out = jnp.where(level_of == 0, 0.0, near(here, -1, 1)) + jnp.where(level_of == levels - 1, 0.0, near(here, 1, 1))
        return [jnp.where(lane < 2 * levels, near(w, 2 * levels, 1), 0.0) for w in weigh(here, out)]

    def stack(tiles):
        return jnp.concatenate(tiles, axis=0)

    def beside(slopes, there):
        straight, slant = [stack([each_slope[i] for each_slope in slopes]) for i in (0, 1)]
        there = stack(there)
        return [jnp.sum((straight if dx == 0 else slant) * near(there, dx, 0), axis=1, keepdims=True) for dx in (-1, 0, 1)]

    inside = [[slope(tile) for tile in column(side)] for side in (0, 1)]
    outside = [slope(beyond(0, dy, 1)) for dy in (-1, 1)]

    even = within(0, REACH)
    for j in range(2, BASE + 8, 2):
        even = even | within(REACH * j, REACH)
    odd = within(REACH, REACH)
    for j in range(3, BASE + 8, 2):
        odd = odd | within(REACH * j, REACH)

    def mix(dx):
        return [jnp.where(first, beyond(dx, 1, 0), beyond(dx, -1, 0)) for first in (even, odd)]

    def extend(j, mine, recv):
        for tile, here in enumerate((recv(0), mine, recv(1))):
            ext[j, tile * rows:(tile + 1) * rows, :cols] = here

    kept = (lane < REACH) | (lane >= 128 - REACH)

    def frame(j, tile, mixed):
        ext[j, tile * rows:(tile + 1) * rows, cols:] = jnp.where(kept, roll(mixed[j % 2], -REACH * j, 1), 0.0)

    mixed = mix(0)
    for j in range(3):
        extend(j, a_send[j], lambda i: a_recv[i, j])
    for j in range(2):
        extend(3 + j, c_send[j], lambda i: c_recv[i, j])
    for j in range(BASE + 8):
        frame(j, 1, mixed)

    each("wait_recv", ("slant",), aslant)
    below, above = ready(corner_row(last)), ready(corner_row(0))
    edges = {
        2 * rows - 1: across(high, above), 2 * rows: across(above, high),
        rows - 1: across(below, low), rows: across(low, below),
    }
    for row in lines:
        lines[row] = [jnp.concatenate(pair, axis=1) for pair in zip(lines[row], edges[row])]
    posts = {1: [], -1: []}
    for side, dy in ((0, -1), (1, 1)):
        tiles = [beyond(dx, dy, 1) for dx in (-1, 0, 1)]
        slopes = [slope(tiles[0]), outside[side], slope(tiles[2])]
        posts[dy].append((cols - 1 if dy > 0 else 0, beside(inside[side], tiles)))
        posts[-dy].append((cols if dy > 0 else cols + 127, beside(slopes, column(side))))
    for tile, dx in ((0, -1), (2, 1)):
        mixed = mix(dx)
        for j in range(BASE + 8):
            frame(j, tile, mixed)
    each("wait_recv", ("coef",), along_x)
    extend(5, k_send[0], lambda i: k_recv[i, 0])
    wide_col = lax.broadcasted_iota(jnp.int32, (3 * rows, cols + 128), 1)
    for d, (dx, dy) in enumerate(DIRS):
        extend(BASE + d, k_send[1 + d], lambda i: k_recv[i, 1 + d])
        if dy != 0:
            whole = ext[BASE + d]
            for spot, parts in posts[dy]:
                whole = whole + jnp.where(wide_col == spot, parts[dx + 1], 0.0)
            ext[BASE + d] = whole
        if dx != 0:
            for row in ((rows - 1, 2 * rows - 1) if dx > 0 else (rows, 2 * rows)):
                ext[BASE + d, row:row + 1, :] = ext[BASE + d, row:row + 1, :] + lines[row][dy + 1]

    def coef(dx, dy):
        return ext[BASE + DIRS.index((dx, dy))]

    shares = (1.0 + cross_share, 1.0 - cross_share)

    def forth(q):
        surface = []
        for c in range(2):
            spread = ext[c] * q
            total = ext[5] * spread
            sums = {1: None, -1: None}
            for dy in (-1, 0, 1):
                turned = near(spread, dy, 1)
                for dx in (-1, 0, 1):
                    if (dx, dy) == (0, 0):
                        continue
                    val = coef(dx, dy) * near(turned, dx, 0)
                    if dx * dy == 0:
                        total = total + val
                    else:
                        sums[dx * dy] = val if sums[dx * dy] is None else sums[dx * dy] + val
            surface.append(total + shares[c] * sums[1] + shares[1 - c] * sums[-1])
        return surface

    def back(q, surface):
        result = regularize(q)
        for c in range(2):
            pull = surface[c]
            scaled = {0: pull, 1: shares[c] * pull, -1: shares[1 - c] * pull}
            basal = ext[5] * pull
            for dy in (-1, 0, 1):
                part = None
                for dx in (-1, 0, 1):
                    if (dx, dy) == (0, 0):
                        continue
                    val = near(coef(-dx, -dy) * scaled[dx * dy], dx, 0)
                    part = val if part is None else part + val
                basal = basal + near(part, dy, 1)
            result = result + ext[c] * basal
        return result

    def regularize(q):
        around = near(q, 1, 0) + near(q, -1, 0) + near(q, 1, 1) + near(q, -1, 1)
        return reg_gamma * (q + reg_smooth * (4.0 * q - around))

    def hessian(q):
        return back(q, forth(q))

    def mine(x):
        return x[rows:2 * rows, :cols]

    image = hessian(ext[2])
    r0 = ext[4] - image
    p0 = ext[3] * r0
    w0 = hessian(p0)
    y0 = ext[3] * w0
    surface = forth(y0)
    curve0 = mine(surface[0]) * mine(surface[0]) + mine(surface[1]) * mine(surface[1]) + mine(y0 * regularize(y0))
    full_y0 = y0
    r0, p0, w0, y0 = mine(r0), mine(p0), mine(w0), mine(y0)

    def total(x):
        return jnp.sum(jnp.sum(x, axis=0, keepdims=True), axis=1, keepdims=True)

    one_lane = lax.broadcasted_iota(jnp.int32, (1, 128), 1)
    sums = jnp.zeros((1, 128), jnp.float32)
    for j, val in enumerate((r0 * p0, p0 * w0, w0 * y0, curve0)):
        sums = jnp.where(one_lane == j, total(val), sums)
    red[...] = sums

    def to_peer(peer):
        return pltpu.make_async_remote_copy(
            src_ref=red, dst_ref=slots.at[me], send_sem=r_send, recv_sem=r_recv,
            device_id=peer, device_id_type=LOGICAL,
        )

    everybody = pltpu.make_async_remote_copy(
        src_ref=slots.at[pl.ds(0, n - 1)], dst_ref=slots.at[pl.ds(0, n - 1)], send_sem=r_send, recv_sem=r_recv,
        device_id=me, device_id_type=LOGICAL,
    )

    def send(j, c):
        peer = jnp.where(2 * me >= n, j, n - 1 - j)

        @pl.when(peer != me)
        def _():
            to_peer(peer).start()
        return c

    for r in range(1, rounds):
        hear(r)
        if r + 1 < rounds:
            herald(r + 1)
    lax.fori_loop(0, n, send, 0, unroll=8)
    u0 = mine(back(full_y0, surface))
    sent_rows = (levels + 2 + 3 * REACH + 2 * (REACH - 2) + 9 * (REACH - 1)) * (cols // 128) + 2 * REACH
    for d in along_x:
        @pl.when(exists(d))
        def _():
            copy(bot.at[0, pl.ds(0, sent_rows)], bot.at[0, pl.ds(0, sent_rows)], d, 0).wait_send()
    each("wait_send", for_y, along_y)
    each("wait_send", ("slant",), aslant)
    everybody.wait_recv()
    slots[me] = sums
    everyone = jnp.sum(slots[...], axis=0)

    def value(j):
        return jnp.sum(jnp.where(one_lane == j, everyone, 0.0), axis=1, keepdims=True)

    rz0, pw, wy, yu = value(0), value(1), value(2), value(3)
    a0 = rz0 / pw
    rz1 = a0 * a0 * wy - rz0
    beta = rz1 / rz0
    more = 1.0 + beta
    curve = more * (more * pw - 2.0 * a0 * wy) + a0 * a0 * yu
    a1 = rz1 / curve
    out_ref[0] = warm_ref[...] + (a0 * p0 + a1 * (more * p0 - a0 * y0))
    out_ref[1] = grad_ref[...] + (-mine(image) - a0 * w0 - a1 * (more * w0 - a0 * u0))
    everybody.wait_send()


def solution(mesh):
    nx, ny = mesh.shape["gx"], mesh.shape["gy"]
    n = nx * ny

    def on_device(gradient, warm_start, viscosity, friction_coef, slide_dir, obs_weight, ice_mask, grounded):
        levels, rows, cols = viscosity.shape
        vmem = pl.BlockSpec(memory_space=pltpu.VMEM)
        f32 = lambda *shape: pltpu.VMEM(shape, jnp.float32)
        flat = (gradient, warm_start, viscosity, friction_coef, slide_dir, obs_weight, ice_mask, grounded)
        out = pl.pallas_call(
            functools.partial(kernel, nx, ny),
            out_shape=f32(2, rows, cols),
            in_specs=[pl.BlockSpec(memory_space=pl.ANY)] * 8,
            out_specs=vmem,
            scratch_shapes=[
                *(pltpu.VMEM(a.shape, a.dtype) for a in flat),
                f32(levels, rows, cols), f32(levels, rows, cols),
                *(f32(cols // 128, levels * rows, 128) for _ in range(2)),
                *(f32(cols // 128, (levels + 2) * rows, 128) for _ in range(2)),
                *(f32(levels, rows, cols) for _ in range(3)),
                *(f32(cols // 128, levels * rows, 128) for _ in range(4)),
                f32(2, rows, cols), f32(2, rows, cols),
                f32(3, rows, cols), f32(2, 3, rows, cols),
                f32(2, rows, cols), f32(2, 2, rows, cols),
                f32(9, rows, cols), f32(2, 9, rows, cols),
                f32(2, 4, rows, 128), f32(2, 4, rows, 128),
                f32(4, 3, rows, 128), f32(4, 3, rows, 128), f32(2, rows, 128), f32(2, 2, rows, 128),
                f32(BASE + 8, 3 * rows, cols + 128),
                f32(1, 128), f32(n, 1, 128),
                pltpu.SemaphoreType.DMA((2,)),
                pltpu.SemaphoreType.DMA((8,)), pltpu.SemaphoreType.DMA((18,)),
                pltpu.SemaphoreType.DMA, pltpu.SemaphoreType.DMA,
                pltpu.SemaphoreType.REGULAR((max(1, (nx - 1).bit_length()), 2)),
            ],
            compiler_params=pltpu.CompilerParams(collective_id=0, has_side_effects=True),
        )(*flat)
        return out[0], out[1]

    flat = P("gx", "gy")
    deep = P(None, "gx", "gy")
    return jax.shard_map(
        on_device,
        mesh=mesh,
        in_specs=(flat, flat, deep, flat, deep, flat, flat, flat),
        out_specs=(flat, flat),
        check_vma=False,
    )
```

```python
import functools

import jax
import jax.numpy as jnp
from jax import lax
from jax.experimental import pallas as pl
from jax.experimental.pallas import tpu as pltpu
from jax.sharding import PartitionSpec as P

vert_coupling = 128.0
sink_rate = 0.0625
bed_drag = 0.5
offset_weight = 0.0019
cross_share = 0.5
reg_gamma = 0.02
reg_smooth = 1.0
diag_scale = 0.003

MESH = pl.DeviceIdType.MESH
LOGICAL = pl.DeviceIdType.LOGICAL
REACH = 6
DIRS = [(-1, 0), (1, 0), (0, -1), (0, 1), (-1, -1), (-1, 1), (1, -1), (1, 1)]
OPPOSITE = [1, 0, 3, 2, 7, 6, 5, 4]
BASE = 6


def roll(x, shift, axis):
    size = x.shape[axis]
    if isinstance(shift, int):
        shift = shift % size
        if shift == 0:
            return x
    return pltpu.roll(x, shift, axis)


def near(x, step, axis):
    return roll(x, -step, axis)


def kernel(
    nx, ny,
    grad_in, warm_in, visc_in, fric_in, slide_in, obs_in, ice_in, ground_in,
    out_ref,
    grad_ref, warm_ref, visc_ref, fric_ref, slide_ref, obs_ref, ice_ref, ground_ref,
    up, down, bot, gbot, top, gtop,
    vx, upx, downx, bx, gx, tx, hx,
    e_send, ef, a_send, a_recv, c_send, c_recv, k_send, k_recv,
    q_send, q_recv, d_send, d_recv, px_send, px_recv,
    ext, red, slots,
    load_sem, s_send, s_recv, r_send, r_recv, entered,
):
    levels, rows, cols = visc_ref.shape
    n = nx * ny
    ix, iy = lax.axis_index("gx"), lax.axis_index("gy")
    me = ix * ny + iy

    loads = [
        pltpu.make_async_copy(src, dst, load_sem.at[min(j, 1)])
        for j, (src, dst) in enumerate((
            (visc_in, visc_ref), (fric_in, fric_ref), (ground_in, ground_ref), (ice_in, ice_ref),
            (slide_in, slide_ref), (obs_in, obs_ref), (warm_in, warm_ref), (grad_in, grad_ref),
        ))
    ]

    def exists(d):
        dx, dy = DIRS[d]
        x, y = ix + dx, iy + dy
        return (x >= 0) & (x < nx) & (y >= 0) & (y < ny)

    barrier = pltpu.get_barrier_semaphore()

    def greet(x, y):
        pl.semaphore_signal(barrier, inc=1, device_id=(x, y), device_id_type=MESH)

    for load in loads:
        load.start()
    expected = ny - 1
    for d in (0, 1):
        expected = expected + exists(d).astype(jnp.int32)

        @pl.when(exists(d))
        def _():
            greet(ix + DIRS[d][0], iy)
    for k in range(1, ny):
        greet(ix, lax.rem(iy + k, ny))
    rounds = entered.shape[0]

    def herald(r):
        for side, step in ((1, -(2 ** r)), (0, 2 ** r)):
            @pl.when((ix + step >= 0) & (ix + step < nx))
            def _():
                pl.semaphore_signal(entered.at[r, side], inc=1, device_id=(ix + step, iy), device_id_type=MESH)

    def hear(r):
        for side, step in ((0, -(2 ** r)), (1, 2 ** r)):
            @pl.when((ix + step >= 0) & (ix + step < nx))
            def _():
                pl.semaphore_wait(entered.at[r, side], 1)

    def copy(src, dst, d, sem):
        dx, dy = DIRS[d]
        return pltpu.make_async_remote_copy(
            src_ref=src, dst_ref=dst,
            send_sem=s_send.at[d], recv_sem=s_recv.at[sem + OPPOSITE[d]],
            device_id=(jnp.clip(ix + dx, 0, nx - 1), jnp.clip(iy + dy, 0, ny - 1)),
            device_id_type=MESH,
        )

    def message(d, what):
        o = OPPOSITE[d]
        dx, dy = DIRS[d]
        side = 0 if dy < 0 else 1

        def part(k):
            return pl.ds(0 if dx < 0 else rows - k, k)

        return {
            "visc": lambda: copy(visc_ref.at[:, part(1), :], vx.at[:, part(1), :], d, 0),
            "slant": lambda: copy(d_send.at[d - 4], d_recv.at[o - 4], d, 0),
            "edge": lambda: copy(e_send.at[:, part(1), :], ef.at[:, part(1), :], d, 0),
            "late": lambda: copy(q_send.at[side], q_recv.at[o - 2], d, 0),
            "side": lambda: copy(px_send.at[:, part(REACH), :], px_recv.at[o, :, part(REACH), :], d, 8),
            "wide": lambda: copy(a_send.at[:, part(REACH), :], a_recv.at[o, :, part(REACH), :], d, 10),
            "less": lambda: copy(c_send.at[:, part(REACH - 2), :], c_recv.at[o, :, part(REACH - 2), :], d, 10),
            "coef": lambda: copy(k_send.at[:, part(REACH - 1), :], k_recv.at[o, :, part(REACH - 1), :], d, 12),
        }[what]()

    along_x, along_y, aslant = (0, 1), (2, 3), (4, 5, 6, 7)
    for_x, for_y = ("visc", "edge", "wide", "less", "side", "coef"), ("late",)

    def each(action, names, towards):
        for name in names:
            for d in towards:
                @pl.when(exists(d))
                def _():
                    if action == "wait_recv":
                        message(OPPOSITE[d], name).wait_recv()
                    elif action == "wait_send":
                        message(d, name).wait_send()
                    else:
                        message(d, name).start()

    def arrive(sem, count):
        block = bot.at[0, pl.ds(0, count * (cols // 128))]
        for d in along_x:
            @pl.when(exists(d))
            def _():
                copy(block, block, OPPOSITE[d], sem).wait_recv()

    def fill(ref, value=0.0):
        ref[...] = jnp.full(ref.shape, value, jnp.float32)

    for d in range(8):
        @pl.when(jnp.logical_not(exists(d)))
        def _():
            if d < 2:
                row = pl.ds(rows - 1 if d == 0 else 0, 1)
                fill(vx.at[:, row, :], 1.0)
                fill(ef.at[:, row, :])
                for ref in (px_recv, a_recv, c_recv, k_recv):
                    fill(ref.at[d])
            elif d < 4:
                fill(q_recv.at[d - 2])
            else:
                fill(d_recv.at[d - 4])

    loads[0].wait()
    pltpu.make_async_copy(visc_in.at[pl.ds(0, 8)], up.at[pl.ds(0, 8)], load_sem.at[1]).wait()

    ice = ice_ref[...].astype(jnp.float32)
    ground = ground_ref[...].astype(jnp.float32)
    fric = fric_ref[...]
    friction = ground * fric
    base = ice * ground * fric
    inverse = 1.0 / (reg_gamma * (1.0 + 4.0 * reg_smooth) + diag_scale * base * fric)
    watch = ice * jnp.sqrt(obs_ref[...])
    turned = base * (0.5 ** 0.5)
    sum_src = turned * (slide_ref[0] + slide_ref[1])
    dif_src = turned * (slide_ref[0] - slide_ref[1])
    lane = lax.broadcasted_iota(jnp.int32, (rows, 128), 1)
    prow = lax.broadcasted_iota(jnp.int32, (rows, 128), 0)

    def factor(v, up, down, drag):
        def eliminate(i, carry):
            e, f = carry
            k = levels - 2 - i
            v_low, v_up = v[i], v[i + 1]
            link = (vert_coupling * 0.5) * (v_low + v_up)
            ratio = link / (link + e)
            up[i] = ratio
            e = sink_rate * v_up + e * ratio
            w_low, w_up = v[k], v[k + 1]
            link = (vert_coupling * 0.5) * (w_low + w_up)
            ratio = link / (link + f)
            down[k] = ratio
            f = sink_rate * w_low + f * ratio
            return e, f

        e = sink_rate * v[0] + drag
        f = sink_rate * v[levels - 1]
        e, f = lax.fori_loop(0, levels - 1, eliminate, (e, f), unroll=True)
        return e, f + drag

    def layer(z):
        return pl.ds(z * rows, rows)

    def put(ref, z, val):
        for c in range(val.shape[1] // 128):
            ref[c, layer(z), :] = val[:, c * 128:(c + 1) * 128]

    def get(ref, z):
        return jnp.concatenate([ref[c, layer(z), :] for c in range(ref.shape[0])], axis=1)

    zero = jnp.zeros((rows, cols), jnp.float32)
    for ref in (top, gtop):
        put(ref, 0, zero)
        put(ref, levels + 1, zero)

    blank = jnp.zeros((rows, 128), jnp.float32)
    def rim(val):
        return jnp.where(lane < 64, val[:, :128], val[:, cols - 128:])

    def within(place, width):
        start = place % 128
        return (lane >= start) & (lane < start + width)

    def pack(fields, place, left, right):
        for val in fields:
            moved = roll(rim(val), place, 1)
            left = jnp.where(within(place, REACH), moved, left)
            right = jnp.where(within(place - REACH, REACH), moved, right)
            place += REACH
        return left, right

    for j, val in enumerate((sum_src, dif_src, warm_ref[...])):
        a_send[j] = val
    for j, val in enumerate((inverse, grad_ref[...])):
        c_send[j] = val
    for j, val in enumerate((friction, watch)):
        e_send[j] = val
    e, f = factor(visc_ref, up, down, bed_drag * friction)
    pl.semaphore_wait(barrier, expected)
    herald(0)
    each("start", ("visc", "edge", "wide", "less"), along_x)
    left, right = blank, blank
    b, t = (0.25 * offset_weight) / f, watch / e
    for z in range(levels):
        k = levels - 1 - z
        v = visc_ref[z]
        g, h = v * b, visc_ref[k] * t
        put(bot, z, b)
        put(gbot, z, g)
        put(top, k + 1, t)
        put(gtop, k + 1, h)
        for place, val in ((z, b), (levels + z, g), (2 * levels + k, h), (3 * levels + k, t)):
            moved = roll(rim(val), place, 1)
            left = jnp.where(lane == place, moved, left)
            right = jnp.where(lane == (place - 1) % 128, moved, right)
        if z < levels - 1:
            t = t * up[k - 1]
            b = b * down[z]
    through = t
    right = roll(right, 1, 1)
    k_send[0] = through
    px_send[0], px_send[1] = left, right
    each("start", ("side",), along_x)
    spans = [(q, tile) for q in range(4) for tile in range(levels // rows)]

    def spot(q, tile):
        return tile * (128 * rows // levels) + REACH * q

    for side in (0, 1):
        q_send[side, 1] = (left, right)[side]
        d_send[side, 1] = (left, right)[side]
        d_send[2 + side, 1] = (left, right)[side]
    for j, row in enumerate((0, rows - 1)):
        corner = [blank, blank]
        for q, tile in spans:
            ref, first = ((bot, 0), (gbot, 0), (gtop, 1), (top, 1))[q]
            span = pl.ds((first + tile * rows) * rows + row, rows, stride=rows)
            place = spot(q, tile)
            moved = roll(jnp.where(lane < 64, ref[0, span, :], ref[cols // 128 - 1, span, :]), place, 1)
            corner[0] = jnp.where(within(place, REACH), moved, corner[0])
            corner[1] = jnp.where(within(place - REACH, REACH), moved, corner[1])
        for side in (0, 1):
            q_send[side, 2 + j] = corner[side]
            d_send[2 * j + side, 2] = corner[side]
    fields = pack((sum_src, dif_src, warm_ref[...], inverse, grad_ref[...], through), 0, blank, blank)

    def weigh(mid, out):
        return 2.0 * mid + out, mid + (2.0 / 3.0) * out

    def gather(z, acc):
        acc = list(acc)
        for ref, other in ((bot, gtop), (gbot, top)):
            straight, slant = weigh(get(other, z + 1), get(other, z) + get(other, z + 2))
            mid = get(ref, z)
            for dy, val in ((-1, near(mid, -1, 1)), (0, mid), (1, near(mid, 1, 1))):
                for dx in (-1, 0, 1):
                    if (dx, dy) != (0, 0):
                        d = DIRS.index((dx, dy))
                        weight = slant if dx * dy != 0 else straight
                        acc[d] = acc[d] + (weight if dx == 0 else near(weight, -dx, 0)) * val
        return tuple(acc)

    row_id = lax.broadcasted_iota(jnp.int32, (rows, cols), 0)
    col_id = lax.broadcasted_iota(jnp.int32, (rows, cols), 1)
    coefs = list(lax.fori_loop(0, levels, gather, (zero,) * 8, unroll=16))
    for d, (dx, dy) in enumerate(DIRS):
        if dx != 0:
            coefs[d] = jnp.where(row_id == (0 if dx < 0 else rows - 1), 0.0, near(coefs[d], dx, 0))
        if dy != 0:
            coefs[d] = jnp.where(col_id == (0 if dy < 0 else cols - 1), 0.0, coefs[d])
        k_send[1 + d] = coefs[d]
    fields = pack(coefs, REACH * BASE, *fields)
    for side in (0, 1):
        q_send[side, 0] = fields[side]
        for j in (0, 1):
            d_send[2 * j + side, 0] = fields[side]
    each("start", ("late",), along_y)
    hear(0)
    each("start", ("slant",), aslant)
    each("start", ("coef",), along_x)
    if rounds > 1:
        herald(1)

    def respond(v, up, down, drag, sight, refs):
        e, f = factor(v, up, down, drag)
        b, t = (0.25 * offset_weight) / f, sight / e
        for z in range(levels):
            k = levels - 1 - z
            put(refs[0], z, b)
            put(refs[1], z, v[z] * b)
            put(refs[2], k, v[k] * t)
            put(refs[3], k, t)
            if z < levels - 1:
                t = t * up[k - 1]
                b = b * down[z]

    far = (bx, gx, hx, tx)
    def strip(ref, row, first=0):
        return jnp.concatenate(
            [ref[c, pl.ds(first * rows + row, levels, stride=rows), :] for c in range(ref.shape[0])], axis=1
        )

    def own_row(row):
        return [strip(bot, row), strip(gbot, row), strip(gtop, row, 1), strip(top, row, 1)]

    def far_row(row):
        return [strip(ref, row) for ref in far]

    phase = lax.rem(lane, 128 * rows // levels)

    def unfold(ahead, behind):
        mixed = []
        for odd in (0, REACH):
            first = (phase >= odd) & (phase < odd + REACH) | (phase >= odd + 2 * REACH) & (phase < odd + 3 * REACH)
            mixed.append(jnp.where(first, ahead, behind))
        return [
            jnp.concatenate([roll(mixed[q % 2], -spot(q, tile), 1) for tile in range(levels // rows)], axis=0)
            for q in range(4)
        ]

    def side_row(row):
        return unfold(*[q_recv[y, 2 if row == 0 else 3] for y in (1, 0)])

    def corner_row(row):
        dx = 1 if row == 0 else -1
        return unfold(*[d_recv[DIRS.index((dx, dy)) - 4, 2] for dy in (1, -1)])

    def level_weights(mid):
        index = lax.broadcasted_iota(jnp.int32, mid.shape, 0)
        out = jnp.where(index == 0, 0.0, near(mid, -1, 0)) + jnp.where(index == levels - 1, 0.0, near(mid, 1, 0))
        return weigh(mid, out)

    def ready(vals):
        moved = [[near(val, dy, 1) for val in vals[:2]] for dy in (-1, 0, 1)]
        return level_weights(vals[2]), level_weights(vals[3]), moved

    def across(here, there):
        width = there[2][0][0].shape[1]
        at = lax.broadcasted_iota(jnp.int32, (1, width), 1)
        parts = []
        for dy in (-1, 0, 1):
            which = 1 if dy != 0 else 0
            by_b, by_g = there[2][dy + 1]
            part = jnp.sum(here[0][which] * by_b + here[1][which] * by_g, axis=0, keepdims=True)
            parts.append(part if dy == 0 else jnp.where(at == (0 if dy < 0 else width - 1), 0.0, part))
        return parts

    last = rows - 1
    low, high = ready(own_row(0)), ready(own_row(last))
    arrive(0, levels + 2)
    respond(vx, upx, downx, bed_drag * ef[0], ef[1], far)
    below, above = ready(far_row(last)), ready(far_row(0))
    lines = {
        2 * rows - 1: across(high, above), 2 * rows: across(above, high),
        rows - 1: across(below, low), rows: across(low, below),
    }
    each("wait_recv", ("side",), along_x)
    arrive(10, 3 * REACH + 2 * (REACH - 2))
    each("wait_recv", ("late",), along_y)
    low, high = ready(side_row(0)), ready(side_row(last))
    level_of = lax.rem(lane, levels)

    def beyond(dx, dy, which):
        return q_recv[0 if dy < 0 else 1, which] if dx == 0 else d_recv[DIRS.index((dx, dy)) - 4, which]

    def column(mine_side):
        return [px_recv[0, mine_side], q_send[mine_side, 1], px_recv[1, mine_side]]

    def slope(here):
        out = jnp.where(level_of == 0, 0.0, near(here, -1, 1)) + jnp.where(level_of == levels - 1, 0.0, near(here, 1, 1))
        return [jnp.where(lane < 2 * levels, near(w, 2 * levels, 1), 0.0) for w in weigh(here, out)]

    def stack(tiles):
        return jnp.concatenate(tiles, axis=0)

    def beside(slopes, there):
        straight, slant = [stack([each_slope[i] for each_slope in slopes]) for i in (0, 1)]
        there = stack(there)
        return [jnp.sum((straight if dx == 0 else slant) * near(there, dx, 0), axis=1, keepdims=True) for dx in (-1, 0, 1)]

    inside = [[slope(tile) for tile in column(side)] for side in (0, 1)]
    outside = [slope(beyond(0, dy, 1)) for dy in (-1, 1)]

    even = within(0, REACH)
    for j in range(2, BASE + 8, 2):
        even = even | within(REACH * j, REACH)
    odd = within(REACH, REACH)
    for j in range(3, BASE + 8, 2):
        odd = odd | within(REACH * j, REACH)

    def mix(dx):
        return [jnp.where(first, beyond(dx, 1, 0), beyond(dx, -1, 0)) for first in (even, odd)]

    def extend(j, mine, recv):
        for tile, here in enumerate((recv(0), mine, recv(1))):
            ext[j, tile * rows:(tile + 1) * rows, :cols] = here

    kept = (lane < REACH) | (lane >= 128 - REACH)

    def frame(j, tile, mixed):
        ext[j, tile * rows:(tile + 1) * rows, cols:] = jnp.where(kept, roll(mixed[j % 2], -REACH * j, 1), 0.0)

    mixed = mix(0)
    for j in range(3):
        extend(j, a_send[j], lambda i: a_recv[i, j])
    for j in range(2):
        extend(3 + j, c_send[j], lambda i: c_recv[i, j])
    for j in range(BASE + 8):
        frame(j, 1, mixed)

    each("wait_recv", ("slant",), aslant)
    below, above = ready(corner_row(last)), ready(corner_row(0))
    edges = {
        2 * rows - 1: across(high, above), 2 * rows: across(above, high),
        rows - 1: across(below, low), rows: across(low, below),
    }
    for row in lines:
        lines[row] = [jnp.concatenate(pair, axis=1) for pair in zip(lines[row], edges[row])]
    posts = {1: [], -1: []}
    for side, dy in ((0, -1), (1, 1)):
        tiles = [beyond(dx, dy, 1) for dx in (-1, 0, 1)]
        slopes = [slope(tiles[0]), outside[side], slope(tiles[2])]
        posts[dy].append((cols - 1 if dy > 0 else 0, beside(inside[side], tiles)))
        posts[-dy].append((cols if dy > 0 else cols + 127, beside(slopes, column(side))))
    for tile, dx in ((0, -1), (2, 1)):
        mixed = mix(dx)
        for j in range(BASE + 8):
            frame(j, tile, mixed)
    each("wait_recv", ("coef",), along_x)
    extend(5, k_send[0], lambda i: k_recv[i, 0])
    wide_col = lax.broadcasted_iota(jnp.int32, (3 * rows, cols + 128), 1)
    for d, (dx, dy) in enumerate(DIRS):
        extend(BASE + d, k_send[1 + d], lambda i: k_recv[i, 1 + d])
        if dy != 0:
            whole = ext[BASE + d]
            for spot, parts in posts[dy]:
                whole = whole + jnp.where(wide_col == spot, parts[dx + 1], 0.0)
            ext[BASE + d] = whole
        if dx != 0:
            for row in ((rows - 1, 2 * rows - 1) if dx > 0 else (rows, 2 * rows)):
                ext[BASE + d, row:row + 1, :] = ext[BASE + d, row:row + 1, :] + lines[row][dy + 1]

    def coef(dx, dy):
        return ext[BASE + DIRS.index((dx, dy))]

    shares = (1.0 + cross_share, 1.0 - cross_share)

    def forth(q):
        surface = []
        for c in range(2):
            spread = ext[c] * q
            total = ext[5] * spread
            sums = {1: None, -1: None}
            for dy in (-1, 0, 1):
                turned = near(spread, dy, 1)
                for dx in (-1, 0, 1):
                    if (dx, dy) == (0, 0):
                        continue
                    val = coef(dx, dy) * near(turned, dx, 0)
                    if dx * dy == 0:
                        total = total + val
                    else:
                        sums[dx * dy] = val if sums[dx * dy] is None else sums[dx * dy] + val
            surface.append(total + shares[c] * sums[1] + shares[1 - c] * sums[-1])
        return surface

    def back(q, surface):
        result = regularize(q)
        for c in range(2):
            pull = surface[c]
            scaled = {0: pull, 1: shares[c] * pull, -1: shares[1 - c] * pull}
            basal = ext[5] * pull
            for dy in (-1, 0, 1):
                part = None
                for dx in (-1, 0, 1):
                    if (dx, dy) == (0, 0):
                        continue
                    val = near(coef(-dx, -dy) * scaled[dx * dy], dx, 0)
                    part = val if part is None else part + val
                basal = basal + near(part, dy, 1)
            result = result + ext[c] * basal
        return result

    def regularize(q):
        around = near(q, 1, 0) + near(q, -1, 0) + near(q, 1, 1) + near(q, -1, 1)
        return reg_gamma * (q + reg_smooth * (4.0 * q - around))

    def hessian(q):
        return back(q, forth(q))

    def mine(x):
        return x[rows:2 * rows, :cols]

    image = hessian(ext[2])
    r0 = ext[4] - image
    p0 = ext[3] * r0
    w0 = hessian(p0)
    y0 = ext[3] * w0
    surface = forth(y0)
    curve0 = mine(surface[0]) * mine(surface[0]) + mine(surface[1]) * mine(surface[1]) + mine(y0 * regularize(y0))
    full_y0 = y0
    r0, p0, w0, y0 = mine(r0), mine(p0), mine(w0), mine(y0)

    def total(x):
        return jnp.sum(jnp.sum(x, axis=0, keepdims=True), axis=1, keepdims=True)

    one_lane = lax.broadcasted_iota(jnp.int32, (1, 128), 1)
    sums = jnp.zeros((1, 128), jnp.float32)
    for j, val in enumerate((r0 * p0, p0 * w0, w0 * y0, curve0)):
        sums = jnp.where(one_lane == j, total(val), sums)
    red[...] = sums

    def to_peer(peer):
        return pltpu.make_async_remote_copy(
            src_ref=red, dst_ref=slots.at[me], send_sem=r_send, recv_sem=r_recv,
            device_id=peer, device_id_type=LOGICAL,
        )

    everybody = pltpu.make_async_remote_copy(
        src_ref=slots.at[pl.ds(0, n - 1)], dst_ref=slots.at[pl.ds(0, n - 1)], send_sem=r_send, recv_sem=r_recv,
        device_id=me, device_id_type=LOGICAL,
    )

    def send(j, c):
        peer = jnp.where(2 * me >= n, j, n - 1 - j)

        @pl.when(peer != me)
        def _():
            to_peer(peer).start()
        return c

    for r in range(1, rounds):
        hear(r)
        if r + 1 < rounds:
            herald(r + 1)
    lax.fori_loop(0, n, send, 0, unroll=8)
    u0 = mine(back(full_y0, surface))
    sent_rows = (levels + 2 + 3 * REACH + 2 * (REACH - 2) + 9 * (REACH - 1)) * (cols // 128) + 2 * REACH
    for d in along_x:
        @pl.when(exists(d))
        def _():
            copy(bot.at[0, pl.ds(0, sent_rows)], bot.at[0, pl.ds(0, sent_rows)], d, 0).wait_send()
    each("wait_send", for_y, along_y)
    each("wait_send", ("slant",), aslant)
    everybody.wait_recv()
    slots[me] = sums
    everyone = jnp.sum(slots[...], axis=0)

    def value(j):
        return jnp.sum(jnp.where(one_lane == j, everyone, 0.0), axis=1, keepdims=True)

    rz0, pw, wy, yu = value(0), value(1), value(2), value(3)
    a0 = rz0 / pw
    rz1 = a0 * a0 * wy - rz0
    beta = rz1 / rz0
    more = 1.0 + beta
    curve = more * (more * pw - 2.0 * a0 * wy) + a0 * a0 * yu
    a1 = rz1 / curve
    out_ref[0] = warm_ref[...] + (a0 * p0 + a1 * (more * p0 - a0 * y0))
    out_ref[1] = grad_ref[...] + (-mine(image) - a0 * w0 - a1 * (more * w0 - a0 * u0))
    everybody.wait_send()


def solution(mesh):
    nx, ny = mesh.shape["gx"], mesh.shape["gy"]
    n = nx * ny

    def on_device(gradient, warm_start, viscosity, friction_coef, slide_dir, obs_weight, ice_mask, grounded):
        levels, rows, cols = viscosity.shape
        vmem = pl.BlockSpec(memory_space=pltpu.VMEM)
        f32 = lambda *shape: pltpu.VMEM(shape, jnp.float32)
        flat = (gradient, warm_start, viscosity, friction_coef, slide_dir, obs_weight, ice_mask, grounded)
        out = pl.pallas_call(
            functools.partial(kernel, nx, ny),
            out_shape=f32(2, rows, cols),
            in_specs=[pl.BlockSpec(memory_space=pl.ANY)] * 8,
            out_specs=vmem,
            scratch_shapes=[
                *(pltpu.VMEM(a.shape, a.dtype) for a in flat),
                f32(levels, rows, cols), f32(levels, rows, cols),
                *(f32(cols // 128, levels * rows, 128) for _ in range(2)),
                *(f32(cols // 128, (levels + 2) * rows, 128) for _ in range(2)),
                *(f32(levels, rows, cols) for _ in range(3)),
                *(f32(cols // 128, levels * rows, 128) for _ in range(4)),
                f32(2, rows, cols), f32(2, rows, cols),
                f32(3, rows, cols), f32(2, 3, rows, cols),
                f32(2, rows, cols), f32(2, 2, rows, cols),
                f32(9, rows, cols), f32(2, 9, rows, cols),
                f32(2, 4, rows, 128), f32(2, 4, rows, 128),
                f32(4, 3, rows, 128), f32(4, 3, rows, 128), f32(2, rows, 128), f32(2, 2, rows, 128),
                f32(BASE + 8, 3 * rows, cols + 128),
                f32(1, 128), f32(n, 1, 128),
                pltpu.SemaphoreType.DMA((2,)),
                pltpu.SemaphoreType.DMA((8,)), pltpu.SemaphoreType.DMA((14,)),
                pltpu.SemaphoreType.DMA, pltpu.SemaphoreType.DMA,
                pltpu.SemaphoreType.REGULAR((max(1, (nx - 1).bit_length()), 2)),
            ],
            compiler_params=pltpu.CompilerParams(collective_id=0, has_side_effects=True),
        )(*flat)
        return out[0], out[1]

    flat = P("gx", "gy")
    deep = P(None, "gx", "gy")
    return jax.shard_map(
        on_device,
        mesh=mesh,
        in_specs=(flat, flat, deep, flat, deep, flat, flat, flat),
        out_specs=(flat, flat),
        check_vma=False,
    )
```
